32 devices in a mesh: slab: 16 (over z, x, core), chan: 2 (over y).
Axes of the slice: x: 2, y: 2, z: 4, core: 2. Of those that a mesh axis runs over, the one named last changes fastest.
Arguments:
- species: int32 [4096], P('slab'), may hold values from 0 to 4
- atom_count: int32 [16], P('slab'), may hold values from 192 to 256, as said below
- halo_index: int32 [16, 2, 128], P('slab'), may hold values from 0 to 255, as said below
- edge_count: int32 [16, 2], P('slab'), may hold values from 512 to 12288, as said below
- inner_edges: int32 [2, 196608], P(None, 'slab'), may hold values from 0 to 255, as said below
- outer_edges: int32 [2, 65536], P(None, 'slab'), may hold values from 0 to 255, as said below
- inner_vec: float32 [3, 196608], P(None, 'slab'), may hold values from -4.8 to 4.8, as said below
- outer_vec: float32 [3, 65536], P(None, 'slab'), may hold values from -4.8 to 4.8, as said below
- embed_table: bfloat16 [64, 5], replicated, may hold values from -6 to 6
- radial_in: bfloat16 [2, 64, 8], replicated, may hold values from -2 to 2
- radial_mid: bfloat16 [2, 64, 64], replicated, may hold values from -0.75 to 0.75
- radial_out: bfloat16 [2, 10, 64, 64], P(None, None, 'chan'), may hold values from -0.75 to 0.75
- mix_in: bfloat16 [2, 3, 64, 64], P(None, None, 'chan'), may hold values from -0.75 to 0.75
- mix_scalar: bfloat16 [2, 192, 64], replicated, may hold values from -0.75 to 0.75
- mix_irrep: bfloat16 [2, 2, 64, 64], replicated, may hold values from -0.75 to 0.75
- readout: float32 [64], replicated, may hold values from -0.75 to 0.75
- species_energy: float32 [5], replicated, may hold values from -6 to -2
Outputs:
- node_state: float32 [9, 64, 4096], P(None, None, 'slab')
- atom_energy: float32 [4096], P('slab')
- mean_energy: float32 [], replicated
The draws below stay inside these ranges and needn't reach their ends.
Inputs may be any that keep to these rules, and one draw needn't show every extreme that they name: `atom_count`: each slab holds between 192 and 256 live atoms (rounded down), live slots first; some slab holds exactly 256. `halo_index`: every entry names a live atom of its own slab. `edge_count`: column 0 lies between 1536 and 12288, column 1 between 512 and 4096 (rounded down); live slots come first in each list; each column reaches its most in some slab. `inner_edges`: both rows name live atoms of the same slab, in every slot. `outer_edges`: row 0 lies below 256; row 1 names a live atom of the slab, in every slot. `inner_vec`: every displacement is shorter than 4.8; nearly all are 0.9 or longer, and a rare few are shorter. `outer_vec`: every displacement is shorter than 4.8; nearly all are 0.9 or longer, and a rare few are shorter.
All inputs are finite; a program needn't handle non-finite values.
Results may differ from the reference program's by a relative error of at most 0.00045.
Values may be sent and summed in bfloat16 or wider, within the bound.
A program may use at most 64 MiB of HBM per device.

```python
import math
import jax
import jax.numpy as jnp
import numpy as np
from jax import lax

C = 64
NB = 8
RH = 64
NPATH = 10
NSPEC = 5
LAYERS = 2
A_DEV = 256
H_DEV = 128
E_IN = 12288
E_OUT = 4096
ATOMS = 4096


def slab_atoms(key):
    base_key = jax.random.fold_in(key, 11)
    slab_total = ATOMS // A_DEV
    counts = jax.random.randint(base_key, (slab_total,), 3 * A_DEV // 4, A_DEV + 1)
    fullest = jax.random.randint(jax.random.fold_in(base_key, 1), (), 0, slab_total)
    return jnp.where(jnp.arange(slab_total) == fullest, A_DEV, counts).astype(jnp.int32)


def live_edges(key, salt, slots):
    base_key = jax.random.fold_in(key, salt)
    slab_total = ATOMS // A_DEV
    counts = jax.random.randint(base_key, (slab_total,), slots // 8, slots + 1)
    fullest = jax.random.randint(jax.random.fold_in(base_key, 1), (), 0, slab_total)
    return jnp.where(jnp.arange(slab_total) == fullest, slots, counts).astype(jnp.int32)


def displacement(key, salt, slots):
    base_key = jax.random.fold_in(key, salt)
    total = slots * (ATOMS // A_DEV)
    heading = jax.random.normal(jax.random.fold_in(base_key, 1), (3, total), jnp.float32)
    radius = jax.random.uniform(jax.random.fold_in(base_key, 2), (total,), jnp.float32, 0.9, 4.8)
    scale = radius / jnp.sqrt(jnp.sum(heading * heading, axis=0) + 0.001)
    return heading * scale[None, :]


def draw_atom_count(key, part):
    return slab_atoms(key)


def draw_halo_index(key, part):
    counts = slab_atoms(key)
    slab_total = ATOMS // A_DEV
    return jax.random.randint(jax.random.fold_in(key, 21), (slab_total, 2, H_DEV), 0, counts[:, None, None]).astype(jnp.int32)


def draw_edge_count(key, part):
    return jnp.stack([live_edges(key, 31, E_IN), live_edges(key, 41, E_OUT)], axis=1)


def draw_inner_edges(key, part):
    counts = slab_atoms(key)
    slab_total = ATOMS // A_DEV
    repeated = jnp.repeat(counts, E_IN, total_repeat_length=slab_total * E_IN)
    return jax.random.randint(jax.random.fold_in(key, 51), (2, slab_total * E_IN), 0, repeated[None, :]).astype(jnp.int32)


def draw_outer_edges(key, part):
    counts = slab_atoms(key)
    slab_total = ATOMS // A_DEV
    repeated = jnp.repeat(counts, E_OUT, total_repeat_length=slab_total * E_OUT)
    halo_slot = jax.random.randint(jax.random.fold_in(key, 61), (slab_total * E_OUT,), 0, 2 * H_DEV)
    targets = jax.random.randint(jax.random.fold_in(key, 62), (slab_total * E_OUT,), 0, repeated)
    return jnp.stack([halo_slot, targets], axis=0).astype(jnp.int32)


def draw_inner_vec(key, part):
    return displacement(key, 71, E_IN)


def draw_outer_vec(key, part):
    return displacement(key, 81, E_OUT)


def with_ends(entries, key, least, largest):
    longest = entries.shape.index(max(entries.shape))
    spots = []
    for shift in (0, 1):
        where = [jax.random.randint(jax.random.fold_in(key, axis), (), 0, length) for axis, length in enumerate(entries.shape)]
        where[longest] = (where[longest] + shift) % entries.shape[longest]
        spots.append(tuple(where))
    return entries.at[spots[0]].set(least).at[spots[1]].set(largest)


def block_scale(key, extent, cuts, low, largest):
    def one(dim, shards_of):
        draws = jax.random.uniform(jax.random.fold_in(jax.random.fold_in(key, 6), dim), (shards_of,), jnp.float32, low / len(cuts), largest / len(cuts))
        return jnp.repeat(jnp.exp(draws), extent[dim] // shards_of).reshape((-1,) + (1,) * (len(extent) - dim - 1))

    level = one(*cuts[0])
    for cut in cuts[1:]:
        level = level * one(*cut)
    return level


def rank_bounds(amount, lean):
    weights = [(1 << 20) // math.isqrt(grade ** lean) + 1 for grade in range(1, amount + 1)]
    width = 1 + sum(weights) // (1 << 30)
    return np.cumsum(np.array([max(1, weight // width) for weight in weights]))


def ranked_ids(own_key, extent, count, skew):
    listing = rank_bounds(count, skew)
    pick = jax.random.randint(jax.random.fold_in(own_key, 1), extent, 0, int(listing[count - 1]))
    grade = jnp.searchsorted(jnp.asarray(listing, jnp.int32), pick, side="right")
    return jax.random.permutation(jax.random.fold_in(own_key, 2), count)[grade].astype(jnp.int32)


def centred(rng, extent, width, reach, cuts=(), kind=jnp.bfloat16):
    gain = block_scale(rng, extent, cuts, -0.22, 0.18) if cuts else 1.0
    values = jax.random.normal(rng, extent, jnp.float32) * width * gain
    return jnp.minimum(jnp.maximum(values, -reach), reach).astype(kind)


def setup_inputs(seed: int = 0) -> dict:
    seeds = jax.random.split(jax.random.key(seed), 18)
    return {
        "species": with_ends(ranked_ids(seeds[0], (ATOMS,), NSPEC, 2), jax.random.fold_in(seeds[0], 3), 0, NSPEC - 1).astype(jnp.int32),
        "atom_count": draw_atom_count(jax.random.fold_in(seeds[17], 71), 0),
        "halo_index": draw_halo_index(jax.random.fold_in(seeds[17], 71), 0),
        "edge_count": draw_edge_count(jax.random.fold_in(seeds[17], 71), 0),
        "inner_edges": draw_inner_edges(jax.random.fold_in(seeds[17], 71), 0),
        "outer_edges": draw_outer_edges(jax.random.fold_in(seeds[17], 71), 0),
        "inner_vec": draw_inner_vec(jax.random.fold_in(seeds[17], 71), 0),
        "outer_vec": draw_outer_vec(jax.random.fold_in(seeds[17], 71), 0),
        "embed_table": centred(seeds[8], (C, NSPEC), 1.0, 6.0),
        "radial_in": centred(seeds[9], (LAYERS, RH, NB), NB ** -0.5, 2.0),
        "radial_mid": centred(seeds[10], (LAYERS, RH, RH), RH ** -0.5, 0.75),
        "radial_out": centred(seeds[11], (LAYERS, NPATH, C, RH), RH ** -0.5, 0.75, ((2, 2),)),
        "mix_in": centred(seeds[12], (LAYERS, 3, C, C), C ** -0.5, 0.75, ((2, 2),)),
        "mix_scalar": centred(seeds[13], (LAYERS, 3 * C, C), C ** -0.5, 0.75),
        "mix_irrep": centred(seeds[14], (LAYERS, 2, C, C), C ** -0.5, 0.75),
        "readout": centred(seeds[15], (C,), C ** -0.5, 0.75, (), jnp.float32),
        "species_energy": jnp.clip(jax.random.uniform(seeds[16], (NSPEC,), jnp.float32, -6.0, -2.0), -6.0, -2.0),
    }


cutoff = 5.0
neighbour_norm = 1.0 / math.sqrt(48.0)
root_three = math.sqrt(3.0)
half_root = 0.5 * math.sqrt(3.0)

def geometry(vectors, basis_total):
    squared = lax.optimization_barrier(jnp.sum(vectors * vectors, axis=0))
    length = jnp.sqrt(squared)
    softened = jnp.sqrt(squared + 0.25)
    directions = vectors / softened[None, :]
    fraction = jnp.minimum(length / cutoff, 1.0)
    envelope = 1.0 - 28.0 * fraction ** 6 + 48.0 * fraction ** 7 - 21.0 * fraction ** 8
    orders = jnp.arange(1, basis_total + 1, dtype=jnp.float32)[:, None]
    bessel = math.sqrt(2.0 / cutoff) * jnp.sin(orders * (math.pi / cutoff) * length[None, :]) / softened[None, :] * envelope[None, :]
    return (directions, bessel)

def edge_messages(source, directions, bessel, live_mask, layer_weights):
    first_layer, middle_layer, last_layer = layer_weights
    hidden = jax.nn.silu(jnp.dot(first_layer, bessel.astype(jnp.bfloat16), preferred_element_type=jnp.float32)).astype(jnp.bfloat16)
    hidden = jax.nn.silu(jnp.dot(middle_layer, hidden, preferred_element_type=jnp.float32)).astype(jnp.bfloat16)
    path_total, channels, breadth = last_layer.shape
    weights = jnp.dot(last_layer.reshape(path_total * channels, breadth), hidden, preferred_element_type=jnp.float32)
    weights = weights.reshape(path_total, channels, hidden.shape[1])
    features = source.astype(jnp.float32)
    scalar_in = features[0]
    vector_in = [features[1], features[2], features[3]]
    tensor_in = [features[4], features[5], features[6], features[7], features[8]]
    unit_parts = [directions[0][None, :], directions[1][None, :], directions[2][None, :]]
    unit_square = unit_parts[0] * unit_parts[0] + unit_parts[1] * unit_parts[1] + unit_parts[2] * unit_parts[2]
    harmonic = [root_three * unit_parts[0] * unit_parts[1], root_three * unit_parts[1] * unit_parts[2], 0.5 * (3.0 * unit_parts[2] * unit_parts[2] - unit_square), root_three * unit_parts[0] * unit_parts[2], half_root * (unit_parts[0] * unit_parts[0] - unit_parts[1] * unit_parts[1])]
    vector_along = vector_in[0] * unit_parts[0] + vector_in[1] * unit_parts[1] + vector_in[2] * unit_parts[2]
    tensor_along = tensor_in[0] * harmonic[0] + tensor_in[1] * harmonic[1] + tensor_in[2] * harmonic[2] + tensor_in[3] * harmonic[3] + tensor_in[4] * harmonic[4]
    out_scalar = weights[0] * scalar_in + weights[1] * tensor_along + weights[2] * vector_along
    cross_term = [vector_in[1] * unit_parts[2] - vector_in[2] * unit_parts[1], vector_in[2] * unit_parts[0] - vector_in[0] * unit_parts[2], vector_in[0] * unit_parts[1] - vector_in[1] * unit_parts[0]]
    gradient = [0.5 * (root_three * tensor_in[0] * unit_parts[1] - tensor_in[2] * unit_parts[0] + root_three * tensor_in[3] * unit_parts[2] + root_three * tensor_in[4] * unit_parts[0]), 0.5 * (root_three * tensor_in[0] * unit_parts[0] + root_three * tensor_in[1] * unit_parts[2] - tensor_in[2] * unit_parts[1] - root_three * tensor_in[4] * unit_parts[1]), 0.5 * (root_three * tensor_in[1] * unit_parts[1] + 2.0 * tensor_in[2] * unit_parts[2] + root_three * tensor_in[3] * unit_parts[0])]
    out_vector = [weights[3] * scalar_in * unit_parts[0] + weights[4] * vector_in[0] + weights[5] * cross_term[0] + weights[6] * gradient[0], weights[3] * scalar_in * unit_parts[1] + weights[4] * vector_in[1] + weights[5] * cross_term[1] + weights[6] * gradient[1], weights[3] * scalar_in * unit_parts[2] + weights[4] * vector_in[2] + weights[5] * cross_term[2] + weights[6] * gradient[2]]
    symmetric = [half_root * (vector_in[0] * unit_parts[1] + vector_in[1] * unit_parts[0]), half_root * (vector_in[1] * unit_parts[2] + vector_in[2] * unit_parts[1]), 0.5 * (3.0 * vector_in[2] * unit_parts[2] - vector_along), half_root * (vector_in[0] * unit_parts[2] + vector_in[2] * unit_parts[0]), half_root * (vector_in[0] * unit_parts[0] - vector_in[1] * unit_parts[1])]
    out_tensor = [weights[7] * scalar_in * harmonic[0] + weights[8] * tensor_in[0] + weights[9] * symmetric[0], weights[7] * scalar_in * harmonic[1] + weights[8] * tensor_in[1] + weights[9] * symmetric[1], weights[7] * scalar_in * harmonic[2] + weights[8] * tensor_in[2] + weights[9] * symmetric[2], weights[7] * scalar_in * harmonic[3] + weights[8] * tensor_in[3] + weights[9] * symmetric[3], weights[7] * scalar_in * harmonic[4] + weights[8] * tensor_in[4] + weights[9] * symmetric[4]]
    stacked = jnp.stack([out_scalar] + out_vector + out_tensor)
    return stacked * live_mask[None, None, :]

def mix_channels(weights, rounded):
    scalar_part = jnp.dot(weights[0], rounded[0], preferred_element_type=jnp.float32)[None]
    vector_part = jnp.einsum('oi,kia->koa', weights[1].astype(jnp.float32), rounded[1:4].astype(jnp.float32))
    tensor_part = jnp.einsum('oi,kia->koa', weights[2].astype(jnp.float32), rounded[4:9].astype(jnp.float32))
    return jnp.concatenate([scalar_part, vector_part, tensor_part], axis=0)

def gate_update(aggregated, scalar_weight, irrep_weight):
    channels = aggregated.shape[1]
    mixed_scalar = jnp.dot(scalar_weight, aggregated[0], preferred_element_type=jnp.float32)
    mixed_vector = jnp.einsum('oi,kia->koa', irrep_weight[0].astype(jnp.float32), aggregated[1:4].astype(jnp.float32))
    mixed_tensor = jnp.einsum('oi,kia->koa', irrep_weight[1].astype(jnp.float32), aggregated[4:9].astype(jnp.float32))
    new_scalar = jax.nn.silu(mixed_scalar[:channels])[None]
    new_vector = jax.nn.sigmoid(mixed_scalar[channels:2 * channels])[None] * mixed_vector
    new_tensor = jax.nn.sigmoid(mixed_scalar[2 * channels:])[None] * mixed_tensor
    return jnp.concatenate([new_scalar, new_vector, new_tensor], axis=0)

def reference(species, atom_count, halo_index, edge_count, inner_edges, outer_edges, inner_vec, outer_vec, embed_table, radial_in, radial_mid, radial_out, mix_in, mix_scalar, mix_irrep, readout, species_energy):
    slab_total = ATOMS // A_DEV
    onehot = species[None, :] == jnp.arange(NSPEC, dtype=jnp.int32)[:, None]
    scalar_init = jnp.dot(embed_table, onehot.astype(jnp.bfloat16), preferred_element_type=jnp.float32)
    node_state = jnp.concatenate([scalar_init[None], jnp.zeros((8, C, ATOMS), jnp.float32)], axis=0)
    offsets = (jnp.arange(slab_total, dtype=jnp.int32) * A_DEV)[:, None]
    inner_source = inner_edges[0].reshape(slab_total, E_IN) + offsets
    inner_target = inner_edges[1].reshape(slab_total, E_IN)
    halo_before = jnp.roll(halo_index, 1, axis=0)[:, 1, :] + jnp.roll(offsets, 1, axis=0)
    halo_after = jnp.roll(halo_index, -1, axis=0)[:, 0, :] + jnp.roll(offsets, -1, axis=0)
    halo_atoms = jnp.concatenate([halo_before, halo_after], axis=1)
    halo_slot = outer_edges[0].reshape(slab_total, E_OUT)
    outer_source = jnp.take_along_axis(halo_atoms, halo_slot, axis=1)
    outer_target = outer_edges[1].reshape(slab_total, E_OUT)
    sources = jnp.concatenate([inner_source, outer_source], axis=1).astype(jnp.int32)
    targets = jnp.concatenate([inner_target, outer_target], axis=1).astype(jnp.int32)
    vectors = jnp.concatenate([inner_vec.reshape(3, slab_total, E_IN), outer_vec.reshape(3, slab_total, E_OUT)], axis=2)
    vectors = jnp.transpose(vectors, (1, 0, 2))
    inner_live = (jnp.arange(E_IN, dtype=jnp.int32)[None, :] < edge_count[:, 0:1]).astype(jnp.float32)
    outer_live = (jnp.arange(E_OUT, dtype=jnp.int32)[None, :] < edge_count[:, 1:2]).astype(jnp.float32)
    live_mask = jnp.concatenate([inner_live, outer_live], axis=1)
    for layer_index in range(LAYERS):
        rounded = node_state.astype(jnp.bfloat16)
        features = mix_channels(mix_in[layer_index], rounded).astype(jnp.bfloat16)
        layer_weights = (radial_in[layer_index], radial_mid[layer_index], radial_out[layer_index])

        def per_slab(carried, pieces):
            slab_sources, slab_targets, slab_vectors, slab_live = pieces
            source = jnp.take(features, slab_sources, axis=2)
            directions, bessel = geometry(slab_vectors, NB)
            message = edge_messages(source, directions, bessel, slab_live, layer_weights)
            summed = jnp.zeros((9, C, A_DEV), jnp.float32).at[:, :, slab_targets].add(message)
            return (carried, summed)
        _, slab_sums = lax.scan(per_slab, jnp.zeros((), jnp.float32), (sources, targets, vectors, live_mask))
        aggregated = jnp.transpose(slab_sums, (1, 2, 0, 3)).reshape(9, C, ATOMS)
        aggregated = (aggregated * neighbour_norm).astype(jnp.bfloat16)
        node_state = node_state + gate_update(aggregated, mix_scalar[layer_index], mix_irrep[layer_index])
    readout_part = lax.optimization_barrier(jnp.sum(node_state[0] * readout[:, None], axis=0))
    species_part = lax.optimization_barrier(jnp.sum(onehot.astype(jnp.float32) * species_energy[:, None], axis=0))
    live_atoms = (jnp.arange(ATOMS, dtype=jnp.int32) % A_DEV < jnp.repeat(atom_count, A_DEV)).astype(jnp.float32)
    atom_energy = (readout_part + species_part) * live_atoms
    mean_energy = jnp.sum(atom_energy) / ATOMS
    return (node_state, atom_energy, mean_energy)
```

```python
import functools
import math

import jax
import jax.numpy as jnp
from jax import lax
from jax.experimental import pallas as pl
from jax.experimental.pallas import tpu as pltpu
from jax.sharding import PartitionSpec as P

cutoff = 5.0
neighbour_norm = 1.0 / math.sqrt(48.0)
root_three = math.sqrt(3.0)
half_root = 0.5 * math.sqrt(3.0)
BLOCK = 2048
WIDE = 4096
TALL, LANES = 16, 128
GROUPS = ((0, 1), (1, 4), (4, 9))
f32 = jnp.float32
bf16 = jnp.bfloat16


def dot(a, b):
    return jnp.dot(a, b, preferred_element_type=f32)


def dot_nt(a, b):
    return lax.dot_general(a, b, (((1,), (1,)), ((), ())), preferred_element_type=f32)


def sigmoid(v):
    return 0.5 * jnp.tanh(0.5 * v) + 0.5


def silu(v):
    half = 0.5 * v
    return half * jnp.tanh(half) + half


def number_rows(rows):
    return lax.broadcasted_iota(jnp.int32, (rows, LANES), 0).astype(f32).astype(bf16)


def onehot_tiles(index, number_ref):
    rows = number_ref.shape[0]
    tiles = []
    for low in range(0, index.shape[1], LANES):
        part = index[:, low : low + LANES].astype(f32)
        part = jnp.broadcast_to(part, (rows, LANES)).astype(bf16)
        tiles.append(jnp.where(number_ref[...] == part, 1.0, 0.0).astype(bf16))
    return jnp.concatenate(tiles, axis=1)


def onehot_rows(index, rows):
    slots = lax.broadcasted_iota(jnp.int32, (rows, index.shape[1]), 0)
    return jnp.where(slots == index, 1.0, 0.0).astype(bf16)


def turned(matrix):
    return matrix.astype(f32).T.astype(bf16)


def initial(embed_ref, species_row):
    return dot(turned(embed_ref[...]), onehot_rows(species_row, embed_ref.shape[0]))


def unit(vec):
    x, y, z = vec[0:1], vec[1:2], vec[2:3]
    squared = x * x + y * y + z * z
    inverse = lax.rsqrt(squared + 0.25)
    return squared, inverse, x * inverse, y * inverse, z * inverse


def bessel_rows(squared, inverse, orders):
    length = jnp.sqrt(squared)
    fraction = jnp.minimum(length * (1.0 / cutoff), 1.0)
    cube = fraction * fraction * fraction
    sixth = cube * cube
    envelope = 1.0 - sixth * (28.0 - fraction * (48.0 - 21.0 * fraction))
    half = length * (0.5 * math.pi / cutoff)
    h2 = half * half
    sine = 1.0
    cosine = 1.0
    for order in range(12, 0, -2):
        sine = 1.0 - sine * h2 * (1.0 / ((order + 1) * order))
        cosine = 1.0 - cosine * h2 * (1.0 / (order * (order - 1)))
    sine = sine * half
    twice_cos = 2.0 - 4.0 * sine * sine
    first = 2.0 * sine * cosine
    scale = math.sqrt(2.0 / cutoff) * inverse * envelope
    before, now = jnp.zeros_like(first), first * scale
    rows = []
    for _ in range(orders):
        rows.append(now)
        before, now = now, twice_cos * now - before
    return jnp.concatenate(rows, axis=0)


def harmonics(x, y, z):
    return [
        root_three * x * y,
        root_three * y * z,
        0.5 * (2.0 * z * z - x * x - y * y),
        root_three * x * z,
        half_root * (x * x - y * y),
    ]


def radial(entry, mid, basis):
    hidden = silu(dot(entry, basis)).astype(bf16)
    return silu(dot(mid, hidden)).astype(bf16)


mesh_ids = pl.DeviceIdType.MESH


def greet(peers):
    barrier = pltpu.get_barrier_semaphore()
    for peer in peers:
        pl.semaphore_signal(barrier, inc=1, device_id=peer, device_id_type=mesh_ids)
    pl.semaphore_wait(barrier, len(peers))


def others(axis, total):
    me = lax.axis_index(axis)
    return [{axis: lax.rem(me + step, total)} for step in range(1, total)]


def beside(total):
    me = lax.axis_index("slab")
    return {"slab": lax.rem(me + total - 1, total)}, {"slab": lax.rem(me + 1, total)}


def remote(src, dst, send_sem, recv_sem, peer):
    return pltpu.make_async_remote_copy(
        src_ref=src,
        dst_ref=dst,
        send_sem=send_sem,
        recv_sem=recv_sem,
        device_id=peer,
        device_id_type=mesh_ids,
    )


def send_halo(send_ref, land_ref, send_sem, recv_sem, total):
    copies = [
        remote(send_ref.at[side], land_ref.at[1 - side], send_sem.at[side], recv_sem.at[side], peer)
        for side, peer in enumerate(beside(total))
    ]
    for copy in copies:
        copy.start()
    return copies


def exchange(agg_ref, all_ref, send_sem, recv_sem, total):
    part = agg_ref.shape[0] // 9
    me = lax.axis_index("chan")
    peers = others("chan", total)
    copies = []
    for k, (low, high) in enumerate(GROUPS):
        span = slice(low * part, high * part)
        for i, peer in enumerate(peers):
            copies.append(
                remote(agg_ref.at[span], all_ref.at[me, span], send_sem.at[i, k], recv_sem.at[i, k], peer)
            )
    for copy in copies:
        copy.start()
    all_ref[me] = agg_ref[...]

    def component(k):
        for group, (low, high) in enumerate(GROUPS):
            if k == low:
                for copy in copies[group * len(peers) : (group + 1) * len(peers)]:
                    copy.wait_recv()
        span = slice(k * part, (k + 1) * part)
        return jnp.concatenate([all_ref[i, span] for i in range(total)], axis=0)

    return copies, component


class Updates:
    def __init__(self, component, scalar, irrep_ref, layer):
        self.component, self.layer, self.irrep = component, layer, irrep_ref
        chans = irrep_ref.shape[2]
        y = dot(scalar, component(0))
        self.scalar = silu(y[:chans])
        self.gates = sigmoid(y[chans : 2 * chans]), sigmoid(y[2 * chans :])

    def __getitem__(self, k):
        if k == 0:
            return self.scalar
        kind = 0 if k < 4 else 1
        return self.gates[kind] * dot(self.irrep[self.layer, kind], self.component(k))


def tall(row):
    return jnp.broadcast_to(row, (TALL, LANES)).astype(bf16)


def kernel(
    slabs,
    parts,
    block,
    wide,
    live_ref,
    count_ref,
    energy_ref,
    species_ref,
    halo_ref,
    inner_edges_ref,
    outer_edges_ref,
    inner_vec_ref,
    outer_vec_ref,
    embed_ref,
    radial_in_ref,
    radial_mid_ref,
    radial_out_ref,
    mix_ref,
    scalar_ref,
    irrep_ref,
    readout_ref,
    state_ref,
    atom_ref,
    mean_ref,
    acc_ref,
    mess_ref,
    source_ref,
    weight_ref,
    basis_ref,
    geo_ref,
    hidden_ref,
    table_ref,
    halo_table_ref,
    first_table_ref,
    paths_ref,
    number_ref,
    agg_ref,
    all_ref,
    send_ref,
    land_ref,
    kind_send_ref,
    kind_land_ref,
    energies_ref,
    kind_send,
    kind_recv,
    agg_send,
    agg_recv,
    halo_send,
    halo_recv,
    energy_send,
    energy_recv,
):
    part = mix_ref.shape[2]
    chans, atoms = state_ref.shape[1:]
    inner_total = inner_edges_ref.shape[1]
    held = halo_ref.shape[1]
    greet(others("chan", parts) + others("slab", slabs))

    values = jnp.broadcast_to(species_ref[...].astype(f32), (16, atoms)).astype(bf16)
    for side in range(2):
        kind_send_ref[side] = dot(values, onehot_rows(halo_ref[side : side + 1], atoms))[0:8]
    kind_copies = send_halo(kind_send_ref, kind_land_ref, kind_send, kind_recv, slabs)

    number_ref[...] = number_rows(atoms)
    start = initial(embed_ref, species_ref[...])
    first_table_ref[0] = dot(mix_ref[0, 0], start.astype(bf16)).astype(bf16)
    for k, path in enumerate((0, 3, 7)):
        paths_ref[k * part : (k + 1) * part] = radial_out_ref[0, path]
    acc_ref[...] = jnp.zeros_like(acc_ref)
    entry = turned(radial_in_ref[0])
    lists = (
        (inner_edges_ref, inner_vec_ref, 0, live_ref[0, 0]),
        (outer_edges_ref, outer_vec_ref, inner_total, live_ref[0, 1]),
    )

    def scatter(edges_ref, span, offset, live):
        lanes = lax.broadcasted_iota(jnp.int32, (1, block), 1) + offset
        target = jnp.where(lanes < live, edges_ref[1:2, span], -1)
        acc_ref[...] += dot_nt(mess_ref[...], onehot_tiles(target, number_ref))

    def first(which, step):
        edges_ref, vec_ref, base, live = lists[which]
        offset = pl.multiple_of(step * block, block)
        span = pl.ds(offset, block)
        place = pl.ds(pl.multiple_of(base + step * block, block), block)
        gathered = dot(first_table_ref[which], onehot_tiles(edges_ref[0:1, span], number_ref))
        squared, inverse, x, y, z = unit(vec_ref[:, span])
        basis = bessel_rows(squared, inverse, radial_in_ref.shape[1]).astype(bf16)
        basis_ref[:, place] = basis
        rows = [x, y, z] + harmonics(x, y, z)
        geo_ref[:, place] = jnp.concatenate(rows, axis=0)
        weights = dot(paths_ref[...], radial(entry, radial_mid_ref[0], basis))
        for lane in range(0, block, LANES):
            cols = slice(lane, lane + LANES)
            around = [tall(row[:, cols]) for row in rows]
            for low in range(0, part, TALL):

                def lead(k):
                    at = slice(k * part + low, k * part + low + TALL)
                    return (weights[at, cols] * gathered[low : low + TALL, cols]).astype(bf16)

                def put(k, value):
                    mess_ref[k * part + low : k * part + low + TALL, cols] = value

                put(0, lead(0))
                for k, (low_k, high_k) in enumerate(GROUPS[1:]):
                    value = lead(1 + k)
                    for j in range(low_k, high_k):
                        put(j, value * around[j - 1])
        scatter(edges_ref, span, offset, live)

    def second(which, step):
        edges_ref, _, base, live = lists[which]
        offset = pl.multiple_of(step * block, block)
        span = pl.ds(offset, block)
        place = pl.ds(pl.multiple_of(base + step * block, block), block)
        features_ref = (table_ref, halo_table_ref)[which]
        source_ref[...] = dot(features_ref[...], onehot_tiles(edges_ref[0:1, span], number_ref)).astype(bf16)
        weight_ref[...] = dot(radial_out, hidden_ref[:, place]).astype(bf16)
        geo = geo_ref[:, place]
        for lane in range(0, block, LANES):
            cols = slice(lane, lane + LANES)
            rows = [geo[k : k + 1, cols] for k in range(8)]
            x, y, z, *q = [tall(row) for row in rows]
            hx, hy, hz = [tall(half_root * row) for row in rows[:3]]
            for low in range(0, part, TALL):

                def at(ref, k):
                    return ref[k * part + low : k * part + low + TALL, cols]

                def put(k, value):
                    mess_ref[k * part + low : k * part + low + TALL, cols] = value

                s = at(source_ref, 0)
                v = [at(source_ref, k) for k in (1, 2, 3)]
                t = [at(source_ref, k) for k in (4, 5, 6, 7, 8)]
                along = v[0] * x + v[1] * y + v[2] * z
                tq = t[0] * q[0] + t[1] * q[1] + t[2] * q[2] + t[3] * q[3] + t[4] * q[4]
                put(0, at(weight_ref, 0) * s + at(weight_ref, 1) * tq + at(weight_ref, 2) * along)
                ws = at(weight_ref, 3) * s
                w4, w5, w6 = at(weight_ref, 4), at(weight_ref, 5), at(weight_ref, 6)
                cross = [
                    v[1] * z - v[2] * y,
                    v[2] * x - v[0] * z,
                    v[0] * y - v[1] * x,
                ]
                t3 = 0.5 * t[2]
                grad = [
                    hy * t[0] - x * t3 + hz * t[3] + hx * t[4],
                    hx * t[0] + hz * t[1] - y * t3 - hy * t[4],
                    hy * t[1] + z * t[2] + hx * t[3],
                ]
                for k, side in enumerate((x, y, z)):
                    put(1 + k, ws * side + w4 * v[k] + w5 * cross[k] + w6 * grad[k])
                ws = at(weight_ref, 7) * s
                w8, w9 = at(weight_ref, 8), at(weight_ref, 9)
                sym = [
                    hy * v[0] + hx * v[1],
                    hz * v[1] + hy * v[2],
                    1.5 * v[2] * z - 0.5 * along,
                    hz * v[0] + hx * v[2],
                    hx * v[0] - hy * v[1],
                ]
                for k in range(5):
                    put(4 + k, ws * q[k] + w8 * t[k] + w9 * sym[k])
        scatter(edges_ref, span, offset, live)

    def sweep(visit, which):
        def body(step, carry):
            visit(which, step)
            return carry

        lax.fori_loop(0, lists[which][0].shape[1] // block, body, 0)

    sweep(first, 0)
    for copy in kind_copies:
        copy.wait()
    kinds = jnp.concatenate([kind_land_ref[0, 0:1], kind_land_ref[1, 0:1]], axis=1).astype(jnp.int32)
    first_table_ref[1] = dot(mix_ref[0, 0], initial(embed_ref, kinds).astype(bf16)).astype(bf16)
    sweep(first, 1)
    agg_ref[0] = (acc_ref[...] * neighbour_norm).astype(bf16)
    copies, component = exchange(agg_ref.at[0], all_ref.at[0], agg_send.at[0], agg_recv.at[0], parts)
    acc_ref[...] = jnp.zeros_like(acc_ref)
    entry_next = turned(radial_in_ref[1])

    def prepare(step, carry):
        span = pl.ds(pl.multiple_of(step * wide, wide), wide)
        hidden_ref[:, span] = radial(entry_next, radial_mid_ref[1], basis_ref[:, span])
        return carry

    lax.fori_loop(0, basis_ref.shape[1] // wide, prepare, 0)
    picks = jnp.concatenate([onehot_rows(halo_ref[side : side + 1], atoms) for side in range(2)], axis=1)
    outs = Updates(component, turned(scalar_ref[0]), irrep_ref, 0)
    for k in range(9):
        out = outs[k]
        if k == 0:
            out += start
        state_ref[k] = out
        which = 0 if k == 0 else (1 if k < 4 else 2)
        span = slice(k * part, (k + 1) * part)
        mixed = dot(mix_ref[1, which], out.astype(bf16)).astype(bf16)
        table_ref[span] = mixed
        picked = dot(mixed, picks).astype(bf16)
        for side in range(2):
            send_ref[side, span] = picked[:, side * held : (side + 1) * held]
    for copy in copies:
        copy.wait_send()
    halo_copies = send_halo(send_ref, land_ref, halo_send, halo_recv, slabs)

    paths, _, breadth = radial_out_ref.shape[1:]
    radial_out = radial_out_ref[1].reshape(paths * part, breadth)
    sweep(second, 0)
    for copy in halo_copies:
        copy.wait()
    for side in range(2):
        halo_table_ref[:, side * held : (side + 1) * held] = land_ref[side]
    sweep(second, 1)
    agg_ref[1] = (acc_ref[...] * neighbour_norm).astype(bf16)
    copies, component = exchange(agg_ref.at[1], all_ref.at[1], agg_send.at[1], agg_recv.at[1], parts)
    lines = lax.broadcasted_iota(jnp.int32, (chans, chans), 0)
    across = lax.broadcasted_iota(jnp.int32, (chans, chans), 1)
    readout = jnp.sum(jnp.where(lines == across, readout_ref[...], 0.0), axis=1, keepdims=True)
    own = jnp.zeros((1, atoms), f32)
    for kind in range(energy_ref.shape[0]):
        own = jnp.where(species_ref[...] == kind, energy_ref[kind], own)
    lanes = lax.broadcasted_iota(jnp.int32, (1, atoms), 1)
    outs = Updates(component, turned(scalar_ref[1]), irrep_ref, 1)
    out = state_ref[0] + outs[0]
    state_ref[0] = out
    total = jnp.sum(out * readout, axis=0, keepdims=True) + own
    total = jnp.where(lanes < count_ref[0], total, 0.0)
    me = lax.axis_index("slab")
    energies_ref[me] = jnp.broadcast_to(jnp.sum(total, axis=1, keepdims=True), energies_ref.shape[1:])
    atom_ref[...] = total
    sums = [
        remote(energies_ref.at[me], energies_ref.at[me], energy_send.at[i], energy_recv.at[i], peer)
        for i, peer in enumerate(others("slab", slabs))
    ]
    for copy in sums:
        copy.start()
    for k in range(1, 9):
        state_ref[k] = state_ref[k] + outs[k]
    for copy in copies:
        copy.wait_send()
    for copy in sums:
        copy.wait()
    mean_ref[...] = jnp.sum(energies_ref[...], axis=0)[0:1, 0:1] * (1.0 / (atoms * slabs))


vmem = pl.BlockSpec(memory_space=pltpu.VMEM)
smem = pl.BlockSpec(memory_space=pltpu.SMEM)


def local(
    species,
    atom_count,
    halo_index,
    edge_count,
    inner_edges,
    outer_edges,
    inner_vec,
    outer_vec,
    embed_table,
    radial_in,
    radial_mid,
    radial_out,
    mix_in,
    mix_scalar,
    mix_irrep,
    readout,
    species_energy,
):
    slabs = lax.axis_size("slab")
    parts = lax.axis_size("chan")
    atoms = species.shape[0]
    chans = embed_table.shape[0]
    part = mix_in.shape[2]
    breadth = radial_mid.shape[1]
    basis = radial_in.shape[2]
    paths = radial_out.shape[1]
    halo = halo_index[0]
    held = halo.shape[1]
    rows = 9 * part
    inner_total, outer_total = inner_edges.shape[1], outer_edges.shape[1]
    total = inner_total + outer_total
    shared = math.gcd(inner_total, outer_total)
    block = math.gcd(BLOCK, shared)
    wide = math.gcd(WIDE, shared)
    dma = pltpu.SemaphoreType.DMA
    node_state, atom_energy, mean_energy = pl.pallas_call(
        functools.partial(kernel, slabs, parts, block, wide),
        out_shape=(
            jax.ShapeDtypeStruct((9, chans, atoms), f32),
            jax.ShapeDtypeStruct((1, atoms), f32),
            jax.ShapeDtypeStruct((1, 1), f32),
        ),
        in_specs=[smem] * 3 + [vmem] * 14,
        out_specs=(vmem, vmem, vmem),
        scratch_shapes=[
            pltpu.VMEM((rows, atoms), f32),
            pltpu.VMEM((rows, block), bf16),
            pltpu.VMEM((rows, block), bf16),
            pltpu.VMEM((paths * part, block), bf16),
            pltpu.VMEM((basis, total), bf16),
            pltpu.VMEM((8, total), f32),
            pltpu.VMEM((breadth, total), bf16),
            pltpu.VMEM((rows, atoms), bf16),
            pltpu.VMEM((rows, 2 * held), bf16),
            pltpu.VMEM((2, part, atoms), bf16),
            pltpu.VMEM((3 * part, breadth), bf16),
            pltpu.VMEM((atoms, LANES), bf16),
            pltpu.VMEM((2, rows, atoms), bf16),
            pltpu.VMEM((2, parts, rows, atoms), bf16),
            pltpu.VMEM((2, rows, held), bf16),
            pltpu.VMEM((2, rows, held), bf16),
            pltpu.VMEM((2, 8, held), f32),
            pltpu.VMEM((2, 8, held), f32),
            pltpu.VMEM((slabs, 8, 128), f32),
            dma((2,)),
            dma((2,)),
            dma((2, parts - 1, 3)),
            dma((2, parts - 1, 3)),
            dma((2,)),
            dma((2,)),
            dma((slabs - 1,)),
            dma((slabs - 1,)),
        ],
        compiler_params=pltpu.CompilerParams(
            vmem_limit_bytes=60 * 1024 * 1024, collective_id=0, has_side_effects=True
        ),
        name="message_passing",
    )(
        edge_count,
        atom_count,
        species_energy,
        species[None, :],
        halo,
        inner_edges,
        outer_edges,
        inner_vec,
        outer_vec,
        embed_table.T,
        jnp.swapaxes(radial_in, 1, 2),
        radial_mid,
        radial_out,
        mix_in,
        jnp.swapaxes(mix_scalar, 1, 2),
        mix_irrep,
        readout[None, :],
    )
    return (node_state, atom_energy[0], mean_energy[0, 0])


def solution(mesh):
    return jax.shard_map(
        local,
        mesh=mesh,
        in_specs=(
            P("slab"),
            P("slab"),
            P("slab", None, None),
            P("slab", None),
            P(None, "slab"),
            P(None, "slab"),
            P(None, "slab"),
            P(None, "slab"),
            P(),
            P(),
            P(),
            P(None, None, "chan", None),
            P(None, None, "chan", None),
            P(),
            P(),
            P(),
            P(),
        ),
        out_specs=(P(None, None, "slab"), P("slab"), P()),
        check_vma=False,
    )
```

```python
import functools
import math

import jax
import jax.numpy as jnp
from jax import lax
from jax.experimental import pallas as pl
from jax.experimental.pallas import tpu as pltpu
from jax.sharding import PartitionSpec as P

cutoff = 5.0
neighbour_norm = 1.0 / math.sqrt(48.0)
root_three = math.sqrt(3.0)
half_root = 0.5 * math.sqrt(3.0)
BLOCK = 2048
WIDE = 4096
TALL, LANES = 16, 128
GROUPS = ((0, 1), (1, 4), (4, 9))
f32 = jnp.float32
bf16 = jnp.bfloat16


def dot(a, b):
    return jnp.dot(a, b, preferred_element_type=f32)


def dot_nt(a, b):
    return lax.dot_general(a, b, (((1,), (1,)), ((), ())), preferred_element_type=f32)


def sigmoid(v):
    return 0.5 * jnp.tanh(0.5 * v) + 0.5


def silu(v):
    half = 0.5 * v
    return half * jnp.tanh(half) + half


def number_rows(rows):
    return lax.broadcasted_iota(jnp.int32, (rows, LANES), 0).astype(f32).astype(bf16)


def onehot_tiles(index, number_ref):
    rows = number_ref.shape[0]
    one, zero = jnp.ones((), bf16), jnp.zeros((), bf16)
    tiles = []
    for low in range(0, index.shape[1], LANES):
        part = index[:, low : low + LANES].astype(f32)
        part = jnp.broadcast_to(part, (rows, LANES)).astype(bf16)
        tiles.append(jnp.where(number_ref[...] == part, one, zero))
    return jnp.concatenate(tiles, axis=1)


def onehot_rows(index, rows):
    slots = lax.broadcasted_iota(jnp.int32, (rows, index.shape[1]), 0)
    return jnp.where(slots == index, 1.0, 0.0).astype(bf16)


def turned(matrix):
    return matrix.astype(f32).T.astype(bf16)


def initial(embed_ref, species_row):
    return dot(turned(embed_ref[...]), onehot_rows(species_row, embed_ref.shape[0]))


def unit(vec):
    x, y, z = vec[0:1], vec[1:2], vec[2:3]
    squared = x * x + y * y + z * z
    inverse = lax.rsqrt(squared + 0.25)
    return squared, inverse, x * inverse, y * inverse, z * inverse


def bessel_rows(squared, inverse, orders):
    length = jnp.sqrt(squared)
    fraction = jnp.minimum(length * (1.0 / cutoff), 1.0)
    cube = fraction * fraction * fraction
    sixth = cube * cube
    envelope = 1.0 - sixth * (28.0 - fraction * (48.0 - 21.0 * fraction))
    half = length * (0.5 * math.pi / cutoff)
    h2 = half * half
    sine = 1.0
    cosine = 1.0
    for order in range(12, 0, -2):
        sine = 1.0 - sine * h2 * (1.0 / ((order + 1) * order))
        cosine = 1.0 - cosine * h2 * (1.0 / (order * (order - 1)))
    sine = sine * half
    twice_cos = 2.0 - 4.0 * sine * sine
    first = 2.0 * sine * cosine
    scale = math.sqrt(2.0 / cutoff) * inverse * envelope
    before, now = jnp.zeros_like(first), first * scale
    rows = []
    for _ in range(orders):
        rows.append(now)
        before, now = now, twice_cos * now - before
    return jnp.concatenate(rows, axis=0)


def harmonics(x, y, z):
    return [
        root_three * x * y,
        root_three * y * z,
        0.5 * (2.0 * z * z - x * x - y * y),
        root_three * x * z,
        half_root * (x * x - y * y),
    ]


def radial(entry, mid, basis):
    hidden = silu(dot(entry, basis)).astype(bf16)
    return silu(dot(mid, hidden)).astype(bf16)


mesh_ids = pl.DeviceIdType.MESH


def greet(peers):
    barrier = pltpu.get_barrier_semaphore()
    for peer in peers:
        pl.semaphore_signal(barrier, inc=1, device_id=peer, device_id_type=mesh_ids)
    pl.semaphore_wait(barrier, len(peers))


def others(axis, total):
    me = lax.axis_index(axis)
    return [{axis: lax.rem(me + step, total)} for step in range(1, total)]


def beside(total):
    me = lax.axis_index("slab")
    return {"slab": lax.rem(me + total - 1, total)}, {"slab": lax.rem(me + 1, total)}


def remote(src, dst, send_sem, recv_sem, peer):
    return pltpu.make_async_remote_copy(
        src_ref=src,
        dst_ref=dst,
        send_sem=send_sem,
        recv_sem=recv_sem,
        device_id=peer,
        device_id_type=mesh_ids,
    )


def send_halo(send_ref, land_ref, send_sem, recv_sem, total):
    copies = [
        remote(send_ref.at[side], land_ref.at[1 - side], send_sem.at[side], recv_sem.at[side], peer)
        for side, peer in enumerate(beside(total))
    ]
    for copy in copies:
        copy.start()
    return copies


def exchange(agg_ref, all_ref, send_sem, recv_sem, total):
    part = agg_ref.shape[0] // 9
    me = lax.axis_index("chan")
    peers = others("chan", total)
    copies = []
    for k, (low, high) in enumerate(GROUPS):
        span = slice(low * part, high * part)
        for i, peer in enumerate(peers):
            copies.append(
                remote(agg_ref.at[span], all_ref.at[me, span], send_sem.at[i, k], recv_sem.at[i, k], peer)
            )
    for copy in copies:
        copy.start()
    all_ref[me] = agg_ref[...]

    def component(k):
        for group, (low, high) in enumerate(GROUPS):
            if k == low:
                for copy in copies[group * len(peers) : (group + 1) * len(peers)]:
                    copy.wait_recv()
        span = slice(k * part, (k + 1) * part)
        return jnp.concatenate([all_ref[i, span] for i in range(total)], axis=0)

    return copies, component


class Updates:
    def __init__(self, component, scalar, irrep_ref, layer):
        self.component, self.layer, self.irrep = component, layer, irrep_ref
        chans = irrep_ref.shape[2]
        y = dot(scalar, component(0))
        self.scalar = silu(y[:chans])
        self.gates = sigmoid(y[chans : 2 * chans]), sigmoid(y[2 * chans :])

    def __getitem__(self, k):
        if k == 0:
            return self.scalar
        kind = 0 if k < 4 else 1
        return self.gates[kind] * dot(self.irrep[self.layer, kind], self.component(k))


def tall(row):
    return jnp.broadcast_to(row, (TALL, LANES)).astype(bf16)


def kernel(slabs, parts, block, wide, *refs):
    radial_out_ref, irrep_ref, state_ref = refs[12], refs[15], refs[17]
    _, paths, part, breadth = radial_out_ref.shape
    atoms = state_ref.shape[2]
    total = refs[5].shape[1] + refs[6].shape[1]
    rows = 9 * part
    pl.run_scoped(
        functools.partial(program, slabs, parts, block, wide, *refs),
        pltpu.VMEM((rows, block), bf16),
        pltpu.VMEM((rows, block), bf16),
        pltpu.VMEM((paths * part, block), bf16),
        pltpu.VMEM((breadth, total), bf16),
        pltpu.VMEM((rows, atoms), bf16),
        pltpu.VMEM((rows, 2 * refs[4].shape[1]), bf16),
        pltpu.VMEM((2, part, atoms), bf16),
        pltpu.VMEM((3 * part, breadth), bf16),
        pltpu.VMEM((atoms, LANES), bf16),
    )


def program(
    slabs,
    parts,
    block,
    wide,
    live_ref,
    count_ref,
    energy_ref,
    species_ref,
    halo_ref,
    inner_edges_ref,
    outer_edges_ref,
    inner_vec_ref,
    outer_vec_ref,
    embed_ref,
    radial_in_ref,
    radial_mid_ref,
    radial_out_ref,
    mix_ref,
    scalar_ref,
    irrep_ref,
    readout_ref,
    state_ref,
    atom_ref,
    mean_ref,
    acc_ref,
    basis_ref,
    geo_ref,
    agg_ref,
    all_ref,
    send_ref,
    land_ref,
    kind_send_ref,
    kind_land_ref,
    energies_ref,
    kind_send,
    kind_recv,
    agg_send,
    agg_recv,
    halo_send,
    halo_recv,
    energy_send,
    energy_recv,
    mess_ref,
    source_ref,
    weight_ref,
    hidden_ref,
    table_ref,
    halo_table_ref,
    first_table_ref,
    paths_ref,
    number_ref,
):
    part = mix_ref.shape[2]
    chans, atoms = state_ref.shape[1:]
    inner_total = inner_edges_ref.shape[1]
    held = halo_ref.shape[1]
    greet(others("chan", parts) + others("slab", slabs))

    values = jnp.broadcast_to(species_ref[...].astype(f32), (16, atoms)).astype(bf16)
    for side in range(2):
        kind_send_ref[side] = dot(values, onehot_rows(halo_ref[side : side + 1], atoms))[0:8]
    kind_copies = send_halo(kind_send_ref, kind_land_ref, kind_send, kind_recv, slabs)

    number_ref[...] = number_rows(atoms)
    start = initial(embed_ref, species_ref[...])
    first_table_ref[0] = dot(mix_ref[0, 0], start.astype(bf16)).astype(bf16)
    for k, path in enumerate((0, 3, 7)):
        paths_ref[k * part : (k + 1) * part] = radial_out_ref[0, path]
    acc_ref[...] = jnp.zeros_like(acc_ref)
    entry = turned(radial_in_ref[0])
    lists = (
        (inner_edges_ref, inner_vec_ref, 0, live_ref[0, 0]),
        (outer_edges_ref, outer_vec_ref, inner_total, live_ref[0, 1]),
    )

    def scatter(edges_ref, span, offset, live):
        lanes = lax.broadcasted_iota(jnp.int32, (1, block), 1) + offset
        target = jnp.where(lanes < live, edges_ref[1:2, span], -1)
        acc_ref[...] += dot_nt(mess_ref[...], onehot_tiles(target, number_ref))

    def first(which, step):
        edges_ref, vec_ref, base, live = lists[which]
        offset = pl.multiple_of(step * block, block)
        span = pl.ds(offset, block)
        place = pl.ds(pl.multiple_of(base + step * block, block), block)
        gathered = dot(first_table_ref[which], onehot_tiles(edges_ref[0:1, span], number_ref))
        squared, inverse, x, y, z = unit(vec_ref[:, span])
        basis = bessel_rows(squared, inverse, radial_in_ref.shape[1]).astype(bf16)
        basis_ref[:, place] = basis
        rows = [x, y, z] + harmonics(x, y, z)
        geo_ref[:, place] = jnp.concatenate(rows, axis=0)
        weights = dot(paths_ref[...], radial(entry, radial_mid_ref[0], basis))
        for lane in range(0, block, LANES):
            cols = slice(lane, lane + LANES)
            around = [tall(row[:, cols]) for row in rows]
            for low in range(0, part, TALL):

                def lead(k):
                    at = slice(k * part + low, k * part + low + TALL)
                    return (weights[at, cols] * gathered[low : low + TALL, cols]).astype(bf16)

                def put(k, value):
                    mess_ref[k * part + low : k * part + low + TALL, cols] = value

                put(0, lead(0))
                for k, (low_k, high_k) in enumerate(GROUPS[1:]):
                    value = lead(1 + k)
                    for j in range(low_k, high_k):
                        put(j, value * around[j - 1])
        scatter(edges_ref, span, offset, live)

    def second(which, step):
        edges_ref, _, base, live = lists[which]
        offset = pl.multiple_of(step * block, block)
        span = pl.ds(offset, block)
        place = pl.ds(pl.multiple_of(base + step * block, block), block)
        features_ref = (table_ref, halo_table_ref)[which]
        source_ref[...] = dot(features_ref[...], onehot_tiles(edges_ref[0:1, span], number_ref)).astype(bf16)
        weight_ref[...] = dot(radial_out, hidden_ref[:, place]).astype(bf16)
        geo = geo_ref[:, place]
        for lane in range(0, block, LANES):
            cols = slice(lane, lane + LANES)
            rows = [geo[k : k + 1, cols] for k in range(8)]
            x, y, z, *q = [tall(row) for row in rows]
            hx, hy, hz = [tall(half_root * row) for row in rows[:3]]
            for low in range(0, part, TALL):

                def at(ref, k):
                    return ref[k * part + low : k * part + low + TALL, cols]

                def put(k, value):
                    mess_ref[k * part + low : k * part + low + TALL, cols] = value

                s = at(source_ref, 0)
                v = [at(source_ref, k) for k in (1, 2, 3)]
                t = [at(source_ref, k) for k in (4, 5, 6, 7, 8)]
                along = v[0] * x + v[1] * y + v[2] * z
                tq = t[0] * q[0] + t[1] * q[1] + t[2] * q[2] + t[3] * q[3] + t[4] * q[4]
                put(0, at(weight_ref, 0) * s + at(weight_ref, 1) * tq + at(weight_ref, 2) * along)
                ws = at(weight_ref, 3) * s
                w4, w5, w6 = at(weight_ref, 4), at(weight_ref, 5), at(weight_ref, 6)
                cross = [
                    v[1] * z - v[2] * y,
                    v[2] * x - v[0] * z,
                    v[0] * y - v[1] * x,
                ]
                t3 = 0.5 * t[2]
                grad = [
                    hy * t[0] - x * t3 + hz * t[3] + hx * t[4],
                    hx * t[0] + hz * t[1] - y * t3 - hy * t[4],
                    hy * t[1] + z * t[2] + hx * t[3],
                ]
                for k, side in enumerate((x, y, z)):
                    put(1 + k, ws * side + w4 * v[k] + w5 * cross[k] + w6 * grad[k])
                ws = at(weight_ref, 7) * s
                w8, w9 = at(weight_ref, 8), at(weight_ref, 9)
                sym = [
                    hy * v[0] + hx * v[1],
                    hz * v[1] + hy * v[2],
                    1.5 * v[2] * z - 0.5 * along,
                    hz * v[0] + hx * v[2],
                    hx * v[0] - hy * v[1],
                ]
                for k in range(5):
                    put(4 + k, ws * q[k] + w8 * t[k] + w9 * sym[k])
        scatter(edges_ref, span, offset, live)

    def sweep(visit, which):
        def body(step, carry):
            visit(which, step)
            return carry

        lax.fori_loop(0, lists[which][0].shape[1] // block, body, 0)

    sweep(first, 0)
    for copy in kind_copies:
        copy.wait()
    kinds = jnp.concatenate([kind_land_ref[0, 0:1], kind_land_ref[1, 0:1]], axis=1).astype(jnp.int32)
    first_table_ref[1] = dot(mix_ref[0, 0], initial(embed_ref, kinds).astype(bf16)).astype(bf16)
    sweep(first, 1)
    agg_ref[0] = (acc_ref[...] * neighbour_norm).astype(bf16)
    copies, component = exchange(agg_ref.at[0], all_ref.at[0], agg_send.at[0], agg_recv.at[0], parts)
    acc_ref[...] = jnp.zeros_like(acc_ref)
    entry_next = turned(radial_in_ref[1])

    def prepare(step, carry):
        span = pl.ds(pl.multiple_of(step * wide, wide), wide)
        hidden_ref[:, span] = radial(entry_next, radial_mid_ref[1], basis_ref[:, span])
        return carry

    lax.fori_loop(0, basis_ref.shape[1] // wide, prepare, 0)
    picks = jnp.concatenate([onehot_rows(halo_ref[side : side + 1], atoms) for side in range(2)], axis=1)
    outs = Updates(component, turned(scalar_ref[0]), irrep_ref, 0)
    for k in range(9):
        out = outs[k]
        if k == 0:
            out += start
        state_ref[k] = out
        which = 0 if k == 0 else (1 if k < 4 else 2)
        span = slice(k * part, (k + 1) * part)
        mixed = dot(mix_ref[1, which], out.astype(bf16)).astype(bf16)
        table_ref[span] = mixed
        picked = dot(mixed, picks).astype(bf16)
        for side in range(2):
            send_ref[side, span] = picked[:, side * held : (side + 1) * held]
    for copy in copies:
        copy.wait_send()
    halo_copies = send_halo(send_ref, land_ref, halo_send, halo_recv, slabs)

    paths, _, breadth = radial_out_ref.shape[1:]
    radial_out = radial_out_ref[1].reshape(paths * part, breadth)
    sweep(second, 0)
    for copy in halo_copies:
        copy.wait()
    for side in range(2):
        halo_table_ref[:, side * held : (side + 1) * held] = land_ref[side]
    sweep(second, 1)
    agg_ref[1] = (acc_ref[...] * neighbour_norm).astype(bf16)
    copies, component = exchange(agg_ref.at[1], all_ref.at[1], agg_send.at[1], agg_recv.at[1], parts)
    lines = lax.broadcasted_iota(jnp.int32, (chans, chans), 0)
    across = lax.broadcasted_iota(jnp.int32, (chans, chans), 1)
    readout = jnp.sum(jnp.where(lines == across, readout_ref[...], 0.0), axis=1, keepdims=True)
    own = jnp.zeros((1, atoms), f32)
    for kind in range(energy_ref.shape[0]):
        own = jnp.where(species_ref[...] == kind, energy_ref[kind], own)
    lanes = lax.broadcasted_iota(jnp.int32, (1, atoms), 1)
    outs = Updates(component, turned(scalar_ref[1]), irrep_ref, 1)
    out = state_ref[0] + outs[0]
    state_ref[0] = out
    total = jnp.sum(out * readout, axis=0, keepdims=True) + own
    total = jnp.where(lanes < count_ref[0], total, 0.0)
    me = lax.axis_index("slab")
    energies_ref[me] = jnp.broadcast_to(jnp.sum(total, axis=1, keepdims=True), energies_ref.shape[1:])
    atom_ref[...] = total
    sums = [
        remote(energies_ref.at[me], energies_ref.at[me], energy_send.at[i], energy_recv.at[i], peer)
        for i, peer in enumerate(others("slab", slabs))
    ]
    for copy in sums:
        copy.start()
    for k in range(1, 9):
        state_ref[k] = state_ref[k] + outs[k]
    for copy in copies:
        copy.wait_send()
    for copy in sums:
        copy.wait()
    mean_ref[...] = jnp.sum(energies_ref[...], axis=0)[0:1, 0:1] * (1.0 / (atoms * slabs))


vmem = pl.BlockSpec(memory_space=pltpu.VMEM)
smem = pl.BlockSpec(memory_space=pltpu.SMEM)


def local(
    species,
    atom_count,
    halo_index,
    edge_count,
    inner_edges,
    outer_edges,
    inner_vec,
    outer_vec,
    embed_table,
    radial_in,
    radial_mid,
    radial_out,
    mix_in,
    mix_scalar,
    mix_irrep,
    readout,
    species_energy,
):
    slabs = lax.axis_size("slab")
    parts = lax.axis_size("chan")
    atoms = species.shape[0]
    chans = embed_table.shape[0]
    part = mix_in.shape[2]
    basis = radial_in.shape[2]
    halo = halo_index[0]
    held = halo.shape[1]
    rows = 9 * part
    inner_total, outer_total = inner_edges.shape[1], outer_edges.shape[1]
    total = inner_total + outer_total
    shared = math.gcd(inner_total, outer_total)
    block = math.gcd(BLOCK, shared)
    wide = math.gcd(WIDE, shared)
    dma = pltpu.SemaphoreType.DMA
    node_state, atom_energy, mean_energy = pl.pallas_call(
        functools.partial(kernel, slabs, parts, block, wide),
        out_shape=(
            jax.ShapeDtypeStruct((9, chans, atoms), f32),
            jax.ShapeDtypeStruct((1, atoms), f32),
            jax.ShapeDtypeStruct((1, 1), f32),
        ),
        in_specs=[smem] * 3 + [vmem] * 14,
        out_specs=(vmem, vmem, vmem),
        scratch_shapes=[
            pltpu.VMEM((rows, atoms), f32),
            pltpu.VMEM((basis, total), bf16),
            pltpu.VMEM((8, total), f32),
            pltpu.VMEM((2, rows, atoms), bf16),
            pltpu.VMEM((2, parts, rows, atoms), bf16),
            pltpu.VMEM((2, rows, held), bf16),
            pltpu.VMEM((2, rows, held), bf16),
            pltpu.VMEM((2, 8, held), f32),
            pltpu.VMEM((2, 8, held), f32),
            pltpu.VMEM((slabs, 8, 128), f32),
            dma((2,)),
            dma((2,)),
            dma((2, parts - 1, 3)),
            dma((2, parts - 1, 3)),
            dma((2,)),
            dma((2,)),
            dma((slabs - 1,)),
            dma((slabs - 1,)),
        ],
        compiler_params=pltpu.CompilerParams(
            vmem_limit_bytes=60 * 1024 * 1024, collective_id=0, has_side_effects=True
        ),
        name="message_passing",
    )(
        edge_count,
        atom_count,
        species_energy,
        species[None, :],
        halo,
        inner_edges,
        outer_edges,
        inner_vec,
        outer_vec,
        embed_table.T,
        jnp.swapaxes(radial_in, 1, 2),
        radial_mid,
        radial_out,
        mix_in,
        jnp.swapaxes(mix_scalar, 1, 2),
        mix_irrep,
        readout[None, :],
    )
    return (node_state, atom_energy[0], mean_energy[0, 0])


def solution(mesh):
    return jax.shard_map(
        local,
        mesh=mesh,
        in_specs=(
            P("slab"),
            P("slab"),
            P("slab", None, None),
            P("slab", None),
            P(None, "slab"),
            P(None, "slab"),
            P(None, "slab"),
            P(None, "slab"),
            P(),
            P(),
            P(),
            P(None, None, "chan", None),
            P(None, None, "chan", None),
            P(),
            P(),
            P(),
            P(),
        ),
        out_specs=(P(None, None, "slab"), P("slab"), P()),
        check_vma=False,
    )
```

```python
import functools
import math

import jax
import jax.numpy as jnp
from jax import lax
from jax.experimental import pallas as pl
from jax.experimental.pallas import tpu as pltpu
from jax.sharding import PartitionSpec as P

cutoff = 5.0
neighbour_norm = 1.0 / math.sqrt(48.0)
root_three = math.sqrt(3.0)
half_root = 0.5 * math.sqrt(3.0)
BLOCK, SUB = 4096, 512
root_third = 1.0 / math.sqrt(3.0)
TALL, LANES = 16, 128
ARRAYS = 14
GROUPS = ((0, 1), (1, 4), (4, 9))
f32 = jnp.float32
bf16 = jnp.bfloat16


def dot(a, b):
    return jnp.dot(a, b, preferred_element_type=f32)


def dot_nt(a, b):
    return lax.dot_general(a, b, (((1,), (1,)), ((), ())), preferred_element_type=f32)


def sigmoid(v):
    return 0.5 * jnp.tanh(0.5 * v) + 0.5


def silu(v):
    half = 0.5 * v
    return half * jnp.tanh(half) + half


def number_rows(rows):
    return lax.broadcasted_iota(jnp.int32, (rows, LANES), 0).astype(f32).astype(bf16)


def onehot_tiles(index, number_ref):
    rows = number_ref.shape[0]
    one, zero = jnp.ones((), bf16), jnp.zeros((), bf16)
    tiles = []
    for low in range(0, index.shape[1], LANES):
        part = index[:, low : low + LANES].astype(f32)
        part = jnp.broadcast_to(part, (rows, LANES)).astype(bf16)
        tiles.append(jnp.where(number_ref[...] == part, one, zero))
    return jnp.concatenate(tiles, axis=1)


def onehot_rows(index, rows):
    slots = lax.broadcasted_iota(jnp.int32, (rows, index.shape[1]), 0)
    return jnp.where(slots == index, 1.0, 0.0).astype(bf16)


def turned(matrix):
    return matrix.astype(f32).T.astype(bf16)


def initial(embed_ref, species_row):
    return dot(turned(embed_ref[...]), onehot_rows(species_row, embed_ref.shape[0]))


def unit(vec):
    x, y, z = vec
    squared = x * x + y * y + z * z
    inverse = lax.rsqrt(squared + 0.25)
    return squared, inverse, x * inverse, y * inverse, z * inverse


def bessel_rows(squared, inverse, orders):
    length = jnp.sqrt(squared)
    fraction = jnp.minimum(length * (1.0 / cutoff), 1.0)
    cube = fraction * fraction * fraction
    sixth = cube * cube
    envelope = 1.0 - sixth * (28.0 - fraction * (48.0 - 21.0 * fraction))
    half = length * (0.5 * math.pi / cutoff)
    h2 = half * half
    sine = 1.0
    cosine = 1.0
    for order in range(12, 0, -2):
        sine = 1.0 - sine * h2 * (1.0 / ((order + 1) * order))
        cosine = 1.0 - cosine * h2 * (1.0 / (order * (order - 1)))
    sine = sine * half
    twice_cos = 2.0 - 4.0 * sine * sine
    first = 2.0 * sine * cosine
    scale = math.sqrt(2.0 / cutoff) * inverse * envelope
    before, now = jnp.zeros_like(first), first * scale
    rows = []
    for _ in range(orders):
        rows.append(now)
        before, now = now, twice_cos * now - before
    return rows


def harmonics(x, y, z):
    return [
        root_three * x * y,
        root_three * y * z,
        0.5 * (2.0 * z * z - x * x - y * y),
        root_three * x * z,
        half_root * (x * x - y * y),
    ]


def radial(entry, mid, basis):
    hidden = silu(dot(entry, basis)).astype(bf16)
    return silu(dot(mid, hidden)).astype(bf16)


mesh_ids = pl.DeviceIdType.MESH


def greet(peers):
    barrier = pltpu.get_barrier_semaphore()
    for peer in peers:
        pl.semaphore_signal(barrier, inc=1, device_id=peer, device_id_type=mesh_ids)
    pl.semaphore_wait(barrier, len(peers))


def others(axis, total):
    me = lax.axis_index(axis)
    return [{axis: lax.rem(me + step, total)} for step in range(1, total)]


def beside(total):
    me = lax.axis_index("slab")
    return {"slab": lax.rem(me + total - 1, total)}, {"slab": lax.rem(me + 1, total)}


def remote(src, dst, send_sem, recv_sem, peer):
    return pltpu.make_async_remote_copy(
        src_ref=src,
        dst_ref=dst,
        send_sem=send_sem,
        recv_sem=recv_sem,
        device_id=peer,
        device_id_type=mesh_ids,
    )


def send_halo(send_ref, land_ref, send_sem, recv_sem, total):
    copies = [
        remote(send_ref.at[side], land_ref.at[1 - side], send_sem.at[side], recv_sem.at[side], peer)
        for side, peer in enumerate(beside(total))
    ]
    for copy in copies:
        copy.start()
    return copies


def exchange(agg_ref, all_ref, send_sem, recv_sem, total):
    part = agg_ref.shape[0] // 9
    me = lax.axis_index("chan")
    peers = others("chan", total)
    copies = []
    for k, (low, high) in enumerate(GROUPS):
        span = slice(low * part, high * part)
        for i, peer in enumerate(peers):
            copies.append(
                remote(agg_ref.at[span], all_ref.at[me, span], send_sem.at[i, k], recv_sem.at[i, k], peer)
            )
    for copy in copies:
        copy.start()
    all_ref[me] = agg_ref[...]

    def component(k):
        for group, (low, high) in enumerate(GROUPS):
            if k == low:
                for copy in copies[group * len(peers) : (group + 1) * len(peers)]:
                    copy.wait_recv()
        span = slice(k * part, (k + 1) * part)
        return jnp.concatenate([all_ref[i, span] for i in range(total)], axis=0)

    return copies, component


class Updates:
    def __init__(self, component, scalar, irrep_ref, layer):
        self.component, self.layer, self.irrep = component, layer, irrep_ref
        chans = irrep_ref.shape[2]
        y = dot(scalar, component(0))
        self.scalar = silu(y[:chans])
        self.gates = sigmoid(y[chans : 2 * chans]), sigmoid(y[2 * chans :])

    def __getitem__(self, k):
        if k == 0:
            return self.scalar
        kind = 0 if k < 4 else 1
        return self.gates[kind] * dot(self.irrep[self.layer, kind], self.component(k))


def tall(row):
    return jnp.broadcast_to(row, (TALL, LANES)).astype(bf16)


def staged(stages, total):
    for time in range(total + len(stages) - 1):
        for late in reversed(range(len(stages))):
            if 0 <= time - late < total:
                stages[late](time - late)


def kernel(slabs, parts, block, *refs):
    halo_ref, inner_edges_ref, outer_edges_ref = refs[4:7]
    radial_out_ref, state_ref = refs[12], refs[17]
    _, paths, part, breadth = radial_out_ref.shape
    atoms = state_ref.shape[2]
    total = inner_edges_ref.shape[1] + outer_edges_ref.shape[1]
    rows = 9 * part
    *refs, sems = refs
    held = refs[-ARRAYS:]
    loads = [
        pltpu.make_async_copy(source, target, sems.at[i])
        for i, (source, target) in enumerate(zip(refs[3 : 3 + ARRAYS], held, strict=True))
    ]
    pl.run_scoped(
        functools.partial(program, slabs, parts, block, loads, *refs[:3], *held, *refs[3 + ARRAYS : -ARRAYS]),
        pltpu.VMEM((rows, block), bf16),
        pltpu.VMEM((rows, block), bf16),
        pltpu.VMEM((paths * part, total), bf16),
        pltpu.VMEM((2, breadth, block), bf16),
        pltpu.VMEM((3 * part, block), bf16),
        pltpu.VMEM((rows, atoms), bf16),
        pltpu.VMEM((rows, 2 * halo_ref.shape[1]), bf16),
        pltpu.VMEM((2, part, atoms), bf16),
        pltpu.VMEM((3 * part, breadth), bf16),
        pltpu.VMEM((atoms, LANES), bf16),
    )


def program(
    slabs,
    parts,
    block,
    loads,
    live_ref,
    count_ref,
    energy_ref,
    species_ref,
    halo_ref,
    inner_edges_ref,
    outer_edges_ref,
    inner_vec_ref,
    outer_vec_ref,
    embed_ref,
    radial_in_ref,
    radial_mid_ref,
    radial_out_ref,
    mix_ref,
    scalar_ref,
    irrep_ref,
    readout_ref,
    state_ref,
    atom_ref,
    mean_ref,
    acc_ref,
    basis_ref,
    geo_ref,
    dense_ref,
    flat_ref,
    agg_ref,
    all_ref,
    send_ref,
    land_ref,
    kind_send_ref,
    kind_land_ref,
    energies_ref,
    kind_send,
    kind_recv,
    agg_send,
    agg_recv,
    halo_send,
    halo_recv,
    energy_send,
    energy_recv,
    mess_ref,
    source_ref,
    weight_ref,
    hidden_ref,
    lead_ref,
    table_ref,
    halo_table_ref,
    first_table_ref,
    paths_ref,
    number_ref,
):
    part = mix_ref.shape[2]
    chans, atoms = state_ref.shape[1:]
    inner_total = inner_edges_ref.shape[1]
    held = halo_ref.shape[1]
    orders = radial_in_ref.shape[1]
    sub = min(SUB, block)
    for load in loads:
        load.start()
    for load in loads[:2]:
        load.wait()
    greet(others("chan", parts) + others("slab", slabs))

    values = jnp.broadcast_to(species_ref[...].astype(f32), (16, atoms)).astype(bf16)
    for side in range(2):
        kind_send_ref[side] = dot(values, onehot_rows(halo_ref[side : side + 1], atoms))[0:8]
    kind_copies = send_halo(kind_send_ref, kind_land_ref, kind_send, kind_recv, slabs)

    for load in loads[2:]:
        load.wait()
    number_ref[...] = number_rows(atoms)
    start = initial(embed_ref, species_ref[...])
    first_table_ref[0] = dot(mix_ref[0, 0], start.astype(bf16)).astype(bf16)
    for k, path in enumerate((0, 3, 7)):
        paths_ref[k * part : (k + 1) * part] = radial_out_ref[0, path]
    acc_ref[...] = jnp.zeros_like(acc_ref)
    lists = (
        (inner_edges_ref, inner_vec_ref, 0, live_ref[0, 0]),
        (outer_edges_ref, outer_vec_ref, inner_total, live_ref[0, 1]),
    )

    def geometry(which):
        _, vec_ref, base, _ = lists[which]
        chunk = 8 * LANES
        many = math.gcd(4, vec_ref.shape[1] // chunk)

        def body(step, carry):
            for part in range(many):
                piece(step * many + part, dense_ref.at[part], flat_ref.at[part])
            return carry

        def piece(step, dense_ref, flat_ref):
            offset = pl.multiple_of(step * chunk, chunk)
            for j in range(8):
                cols = pl.ds(pl.multiple_of(offset + j * LANES, LANES), LANES)
                for axis in range(3):
                    dense_ref[axis * 8 + j : axis * 8 + j + 1] = vec_ref[axis : axis + 1, cols]
            squared, inverse, x, y, z = unit([dense_ref[8 * axis : 8 * axis + 8] for axis in range(3)])
            rows = bessel_rows(squared, inverse, orders) + [x, y, z] + harmonics(x, y, z)
            for k, row in enumerate(rows):
                flat_ref[8 * k : 8 * k + 8] = row
            for j in range(8):
                cols = pl.ds(pl.multiple_of(base + offset + j * LANES, LANES), LANES)
                basis_ref[:, cols] = flat_ref[pl.ds(j, orders, stride=8)].astype(bf16)
                geo_ref[:, cols] = flat_ref[pl.ds(8 * orders + j, 8, stride=8)]

        lax.fori_loop(0, vec_ref.shape[1] // (many * chunk), body, 0)

    def hidden(layer, entry, place):
        hidden_ref[0] = silu(dot(entry, basis_ref[:, place])).astype(bf16)
        hidden_ref[1] = silu(dot(radial_mid_ref[layer], hidden_ref[0])).astype(bf16)

    def sweep(make, which):
        edges_ref, _, base, live = lists[which]

        def body(step, carry):
            offset = step * block

            def span(j):
                return pl.ds(pl.multiple_of(offset + j * sub, sub), sub)

            def place(j):
                return pl.ds(pl.multiple_of(base + offset + j * sub, sub), sub)

            def scatter(j):
                lanes = lax.broadcasted_iota(jnp.int32, (1, sub), 1) + (offset + j * sub)
                target = jnp.where(lanes < live, edges_ref[1:2, span(j)], -1)
                acc_ref[...] += dot_nt(mess_ref[:, j * sub : (j + 1) * sub], onehot_tiles(target, number_ref))

            def gather(j, features):
                return dot(features, onehot_tiles(edges_ref[0:1, span(j)], number_ref)).astype(bf16)

            make(which, pl.ds(pl.multiple_of(base + offset, block), block), place, gather, scatter)
            return carry

        lax.fori_loop(0, edges_ref.shape[1] // block, body, 0)

    entry = turned(radial_in_ref[0])

    def first(which, whole, place, gather, scatter):
        hidden(0, entry, whole)
        for j in range(block // sub):
            source_ref[0:part, j * sub : (j + 1) * sub] = gather(j, first_table_ref[which])
        lead_ref[...] = dot(paths_ref[...], hidden_ref[1]).astype(bf16)

        def combine(j):
            geo = geo_ref[:, place(j)]
            for lane in range(0, sub, LANES):
                cols = slice(j * sub + lane, j * sub + lane + LANES)
                around = [tall(geo[k : k + 1, lane : lane + LANES]) for k in range(8)]
                for low in range(0, part, TALL):
                    held = source_ref[low : low + TALL, cols]

                    def lead(k):
                        return lead_ref[k * part + low : k * part + low + TALL, cols] * held

                    def put(k, value):
                        mess_ref[k * part + low : k * part + low + TALL, cols] = value

                    put(0, lead(0))
                    for k, (low_k, high_k) in enumerate(GROUPS[1:]):
                        value = lead(1 + k)
                        for i in range(low_k, high_k):
                            put(i, value * around[i - 1])

        staged([combine, scatter], block // sub)

    def second(which, whole, place, gather, scatter):
        features_ref = (table_ref, halo_table_ref)[which]

        def fetch(j):
            source_ref[:, j * sub : (j + 1) * sub] = gather(j, features_ref[...])

        def combine(j):
            geo = geo_ref[:, place(j)]
            for lane in range(0, sub, LANES):
                cols = slice(j * sub + lane, j * sub + lane + LANES)
                x, y, z, *q = [tall(geo[k : k + 1, lane : lane + LANES]) for k in range(8)]
                weighed = pl.ds(pl.multiple_of(place(j).start + lane, LANES), LANES)
                for low in range(0, part, TALL):

                    def at(k):
                        return source_ref[k * part + low : k * part + low + TALL, cols]

                    def path(k):
                        return weight_ref[k * part + low : k * part + low + TALL, weighed]

                    def put(k, value):
                        mess_ref[k * part + low : k * part + low + TALL, cols] = value

                    s = at(0)
                    v = [at(k) for k in (1, 2, 3)]
                    t = [at(k) for k in (4, 5, 6, 7, 8)]
                    a, b, c = v[0] * x, v[1] * y, v[2] * z
                    flat = a + b
                    along = flat + c
                    pairs = [
                        (v[1] * z, v[2] * y),
                        (v[2] * x, v[0] * z),
                        (v[0] * y, v[1] * x),
                    ]
                    third = root_third * t[2]
                    grad = [
                        y * t[0] + z * t[3] + x * (t[4] - third),
                        x * t[0] + z * t[1] - y * (t[4] + third),
                        y * t[1] + x * t[3] + z * (third + third),
                    ]
                    tq = x * grad[0] + y * grad[1] + z * grad[2]
                    put(0, path(0) * s + path(1) * tq + path(2) * along)
                    ws = path(3) * s
                    w4, w5, w6 = path(4), path(5), path(6)
                    for k, side in enumerate((x, y, z)):
                        one, two = pairs[k]
                        put(1 + k, ws * side + w4 * v[k] + w5 * (one - two) + w6 * grad[k])
                    ws = path(7) * s
                    w8, w9 = path(8), path(9)
                    sums = [one + two for one, two in pairs]
                    sym = [sums[2], sums[0], (2.0 * root_third) * c - root_third * flat, sums[1], a - b]
                    for k in range(5):
                        put(4 + k, ws * q[k] + w8 * t[k] + w9 * sym[k])

        staged([fetch, combine, scatter], block // sub)

    geometry(0)
    geometry(1)
    sweep(first, 0)
    for copy in kind_copies:
        copy.wait()
    kinds = jnp.concatenate([kind_land_ref[0, 0:1], kind_land_ref[1, 0:1]], axis=1).astype(jnp.int32)
    first_table_ref[1] = dot(mix_ref[0, 0], initial(embed_ref, kinds).astype(bf16)).astype(bf16)
    sweep(first, 1)
    agg_ref[0] = (acc_ref[...] * neighbour_norm).astype(bf16)
    copies, component = exchange(agg_ref.at[0], all_ref.at[0], agg_send.at[0], agg_recv.at[0], parts)
    acc_ref[...] = jnp.zeros_like(acc_ref)
    entry_next = turned(radial_in_ref[1])
    paths = radial_out_ref.shape[1]

    def prepare(step, carry):
        whole = pl.ds(pl.multiple_of(step * block, block), block)
        hidden(1, entry_next, whole)
        for path in range(paths):
            weighed = dot(radial_out_ref[1, path], hidden_ref[1])
            if path in (1, 6, 9):
                weighed = weighed * half_root
            weight_ref[path * part : (path + 1) * part, whole] = weighed.astype(bf16)
        return carry

    lax.fori_loop(0, basis_ref.shape[1] // block, prepare, 0)
    picks = jnp.concatenate([onehot_rows(halo_ref[side : side + 1], atoms) for side in range(2)], axis=1)
    outs = Updates(component, turned(scalar_ref[0]), irrep_ref, 0)
    for k in range(9):
        out = outs[k]
        if k == 0:
            out += start
        state_ref[k] = out
        which = 0 if k == 0 else (1 if k < 4 else 2)
        table_ref[k * part : (k + 1) * part] = dot(mix_ref[1, which], out.astype(bf16)).astype(bf16)
    picked = dot(table_ref[...], picks).astype(bf16)
    for side in range(2):
        send_ref[side] = picked[:, side * held : (side + 1) * held]
    for copy in copies:
        copy.wait_send()
    halo_copies = send_halo(send_ref, land_ref, halo_send, halo_recv, slabs)

    sweep(second, 0)
    for copy in halo_copies:
        copy.wait()
    for side in range(2):
        halo_table_ref[:, side * held : (side + 1) * held] = land_ref[side]
    sweep(second, 1)
    agg_ref[1] = (acc_ref[...] * neighbour_norm).astype(bf16)
    copies, component = exchange(agg_ref.at[1], all_ref.at[1], agg_send.at[1], agg_recv.at[1], parts)
    lines = lax.broadcasted_iota(jnp.int32, (chans, chans), 0)
    across = lax.broadcasted_iota(jnp.int32, (chans, chans), 1)
    readout = jnp.sum(jnp.where(lines == across, readout_ref[...], 0.0), axis=1, keepdims=True)
    own = jnp.zeros((1, atoms), f32)
    for kind in range(energy_ref.shape[0]):
        own = jnp.where(species_ref[...] == kind, energy_ref[kind], own)
    lanes = lax.broadcasted_iota(jnp.int32, (1, atoms), 1)
    outs = Updates(component, turned(scalar_ref[1]), irrep_ref, 1)
    out = state_ref[0] + outs[0]
    state_ref[0] = out
    total = jnp.sum(out * readout, axis=0, keepdims=True) + own
    total = jnp.where(lanes < count_ref[0, 0], total, 0.0)
    me = lax.axis_index("slab")
    energies_ref[me] = jnp.broadcast_to(jnp.sum(total, axis=1, keepdims=True), energies_ref.shape[1:])
    atom_ref[...] = total
    sums = [
        remote(energies_ref.at[me], energies_ref.at[me], energy_send.at[i], energy_recv.at[i], peer)
        for i, peer in enumerate(others("slab", slabs))
    ]
    for copy in sums:
        copy.start()
    for k in range(1, 9):
        state_ref[k] = state_ref[k] + outs[k]
    for copy in copies:
        copy.wait_send()
    for copy in sums:
        copy.wait()
    mean_ref[...] = jnp.sum(energies_ref[...], axis=0)[0:1, 0:1] * (1.0 / (atoms * slabs))


def deliver(state_in_ref, atom_in_ref, mean_in_ref, state_ref, atom_ref, mean_ref):
    state_ref[...] = state_in_ref[...]
    atom_ref[...] = atom_in_ref[...]
    mean_ref[...] = mean_in_ref[...]


vmem = pl.BlockSpec(memory_space=pltpu.VMEM)
smem = pl.BlockSpec(memory_space=pltpu.SMEM)


def local(
    species,
    atom_count,
    halo_index,
    edge_count,
    inner_edges,
    outer_edges,
    inner_vec,
    outer_vec,
    embed_table,
    radial_in,
    radial_mid,
    radial_out,
    mix_in,
    mix_scalar,
    mix_irrep,
    readout,
    species_energy,
):
    slabs = lax.axis_size("slab")
    parts = lax.axis_size("chan")
    atoms = species.shape[0]
    chans = embed_table.shape[0]
    part = mix_in.shape[2]
    basis = radial_in.shape[2]
    halo = halo_index[0]
    held = halo.shape[1]
    rows = 9 * part
    inner_total, outer_total = inner_edges.shape[1], outer_edges.shape[1]
    total = inner_total + outer_total
    shared = math.gcd(inner_total, outer_total)
    block = math.gcd(BLOCK, shared)
    dma = pltpu.SemaphoreType.DMA
    arrays = (
        species[None, :],
        halo,
        inner_edges,
        outer_edges,
        inner_vec,
        outer_vec,
        embed_table.T,
        jnp.swapaxes(radial_in, 1, 2),
        radial_mid,
        radial_out,
        mix_in,
        jnp.swapaxes(mix_scalar, 1, 2),
        mix_irrep,
        readout[None, :],
    )
    shapes = (
        jax.ShapeDtypeStruct((9, chans, atoms), f32),
        jax.ShapeDtypeStruct((1, atoms), f32),
        jax.ShapeDtypeStruct((1, 1), f32),
    )
    results = pl.pallas_call(
        functools.partial(kernel, slabs, parts, block),
        out_shape=shapes,
        in_specs=[smem] * 3 + [pl.BlockSpec(memory_space=pltpu.HBM)] * ARRAYS,
        out_specs=(vmem, vmem, vmem),
        scratch_shapes=[
            pltpu.VMEM((rows, atoms), f32),
            pltpu.VMEM((basis, total), bf16),
            pltpu.VMEM((8, total), f32),
            pltpu.VMEM((4, 24, LANES), f32),
            pltpu.VMEM((4, 8 * (basis + 8), LANES), f32),
            pltpu.VMEM((2, rows, atoms), bf16),
            pltpu.VMEM((2, parts, rows, atoms), bf16),
            pltpu.VMEM((2, rows, held), bf16),
            pltpu.VMEM((2, rows, held), bf16),
            pltpu.VMEM((2, 8, held), f32),
            pltpu.VMEM((2, 8, held), f32),
            pltpu.VMEM((slabs, 8, 128), f32),
            dma((2,)),
            dma((2,)),
            dma((2, parts - 1, 3)),
            dma((2, parts - 1, 3)),
            dma((2,)),
            dma((2,)),
            dma((slabs - 1,)),
            dma((slabs - 1,)),
            *[pltpu.VMEM(array.shape, array.dtype) for array in arrays],
            dma((ARRAYS,)),
        ],
        compiler_params=pltpu.CompilerParams(
            vmem_limit_bytes=60 * 1024 * 1024, collective_id=0, has_side_effects=True
        ),
        name="message_passing",
    )(
        edge_count,
        atom_count[None, :],
        species_energy,
        *arrays,
    )
    node_state, atom_energy, mean_energy = pl.pallas_call(
        deliver,
        out_shape=shapes,
        in_specs=[vmem] * 3,
        out_specs=(vmem,) * 3,
        compiler_params=pltpu.CompilerParams(vmem_limit_bytes=8 * 1024 * 1024),
        name="deliver",
    )(*results)
    return (node_state, atom_energy[0], mean_energy[0, 0])


def solution(mesh):
    return jax.shard_map(
        local,
        mesh=mesh,
        in_specs=(
            P("slab"),
            P("slab"),
            P("slab", None, None),
            P("slab", None),
            P(None, "slab"),
            P(None, "slab"),
            P(None, "slab"),
            P(None, "slab"),
            P(),
            P(),
            P(),
            P(None, None, "chan", None),
            P(None, None, "chan", None),
            P(),
            P(),
            P(),
            P(),
        ),
        out_specs=(P(None, None, "slab"), P("slab"), P()),
        check_vma=False,
    )
```

```python
import functools
import math

import jax
import jax.numpy as jnp
from jax import lax
from jax.experimental import pallas as pl
from jax.experimental.pallas import tpu as pltpu
from jax.sharding import PartitionSpec as P

cutoff = 5.0
neighbour_norm = 1.0 / math.sqrt(48.0)
root_three = math.sqrt(3.0)
half_root = 0.5 * math.sqrt(3.0)
BLOCK, SUB = 4096, 512
root_third = 1.0 / math.sqrt(3.0)
TALL, LANES = 16, 128
ARRAYS = 14
GROUPS = ((0, 1), (1, 4), (4, 9))
f32 = jnp.float32
bf16 = jnp.bfloat16


def dot(a, b):
    return jnp.dot(a, b, preferred_element_type=f32)


def dot_nt(a, b):
    return lax.dot_general(a, b, (((1,), (1,)), ((), ())), preferred_element_type=f32)


def sigmoid(v):
    return 0.5 * jnp.tanh(0.5 * v) + 0.5


def silu(v):
    half = 0.5 * v
    return half * jnp.tanh(half) + half


def number_rows(rows):
    return lax.broadcasted_iota(jnp.int32, (rows, LANES), 0).astype(f32).astype(bf16)


def onehot_tiles(index, number_ref):
    rows = number_ref.shape[0]
    one, zero = jnp.ones((), bf16), jnp.zeros((), bf16)
    tiles = []
    for low in range(0, index.shape[1], LANES):
        part = index[:, low : low + LANES].astype(f32)
        part = jnp.broadcast_to(part, (rows, LANES)).astype(bf16)
        tiles.append(jnp.where(number_ref[...] == part, one, zero))
    return jnp.concatenate(tiles, axis=1)


def onehot_rows(index, rows):
    slots = lax.broadcasted_iota(jnp.int32, (rows, index.shape[1]), 0)
    return jnp.where(slots == index, 1.0, 0.0).astype(bf16)


def turned(matrix):
    return matrix.astype(f32).T.astype(bf16)


def initial(embed_ref, species_row):
    return dot(turned(embed_ref[...]), onehot_rows(species_row, embed_ref.shape[0]))


def unit(vec):
    x, y, z = vec
    squared = x * x + y * y + z * z
    inverse = lax.rsqrt(squared + 0.25)
    return squared, inverse, x * inverse, y * inverse, z * inverse


def bessel_rows(squared, inverse, orders):
    length = jnp.sqrt(squared)
    fraction = jnp.minimum(length * (1.0 / cutoff), 1.0)
    cube = fraction * fraction * fraction
    sixth = cube * cube
    envelope = 1.0 - sixth * (28.0 - fraction * (48.0 - 21.0 * fraction))
    half = length * (0.5 * math.pi / cutoff)
    h2 = half * half
    sine = 1.0
    cosine = 1.0
    for order in range(12, 0, -2):
        sine = 1.0 - sine * h2 * (1.0 / ((order + 1) * order))
        cosine = 1.0 - cosine * h2 * (1.0 / (order * (order - 1)))
    sine = sine * half
    twice_cos = 2.0 - 4.0 * sine * sine
    first = 2.0 * sine * cosine
    scale = math.sqrt(2.0 / cutoff) * inverse * envelope
    before, now = jnp.zeros_like(first), first * scale
    rows = []
    for _ in range(orders):
        rows.append(now)
        before, now = now, twice_cos * now - before
    return rows


def harmonics(x, y, z):
    return [
        root_three * x * y,
        root_three * y * z,
        0.5 * (2.0 * z * z - x * x - y * y),
        root_three * x * z,
        half_root * (x * x - y * y),
    ]


def radial(entry, mid, basis):
    hidden = silu(dot(entry, basis)).astype(bf16)
    return silu(dot(mid, hidden)).astype(bf16)


mesh_ids = pl.DeviceIdType.MESH


def greet(peers):
    barrier = pltpu.get_barrier_semaphore()
    for peer in peers:
        pl.semaphore_signal(barrier, inc=1, device_id=peer, device_id_type=mesh_ids)
    pl.semaphore_wait(barrier, len(peers))


def others(axis, total):
    me = lax.axis_index(axis)
    return [{axis: lax.rem(me + step, total)} for step in range(1, total)]


def beside(total):
    me = lax.axis_index("slab")
    return {"slab": lax.rem(me + total - 1, total)}, {"slab": lax.rem(me + 1, total)}


def remote(src, dst, send_sem, recv_sem, peer):
    return pltpu.make_async_remote_copy(
        src_ref=src,
        dst_ref=dst,
        send_sem=send_sem,
        recv_sem=recv_sem,
        device_id=peer,
        device_id_type=mesh_ids,
    )


def send_halo(send_ref, land_ref, send_sem, recv_sem, total):
    copies = [
        remote(send_ref.at[side], land_ref.at[1 - side], send_sem.at[side], recv_sem.at[side], peer)
        for side, peer in enumerate(beside(total))
    ]
    for copy in copies:
        copy.start()
    return copies


def exchange(agg_ref, all_ref, send_sem, recv_sem, total):
    part = agg_ref.shape[0] // 9
    me = lax.axis_index("chan")
    peers = others("chan", total)
    copies = []
    for k, (low, high) in enumerate(GROUPS):
        span = slice(low * part, high * part)
        for i, peer in enumerate(peers):
            copies.append(
                remote(agg_ref.at[span], all_ref.at[me, span], send_sem.at[i, k], recv_sem.at[i, k], peer)
            )
    for copy in copies:
        copy.start()
    all_ref[me] = agg_ref[...]

    def component(k):
        for group, (low, high) in enumerate(GROUPS):
            if k == low:
                for copy in copies[group * len(peers) : (group + 1) * len(peers)]:
                    copy.wait_recv()
        span = slice(k * part, (k + 1) * part)
        return jnp.concatenate([all_ref[i, span] for i in range(total)], axis=0)

    return copies, component


def settled(all_ref):
    part = all_ref.shape[1] // 9

    def component(k):
        span = slice(k * part, (k + 1) * part)
        return jnp.concatenate([all_ref[i, span] for i in range(all_ref.shape[0])], axis=0)

    return component


class Updates:
    def __init__(self, component, scalar, irrep_ref, layer):
        self.component, self.layer, self.irrep = component, layer, irrep_ref
        chans = irrep_ref.shape[2]
        y = dot(scalar, component(0))
        self.scalar = silu(y[:chans])
        self.gates = sigmoid(y[chans : 2 * chans]), sigmoid(y[2 * chans :])

    def __getitem__(self, k):
        if k == 0:
            return self.scalar
        kind = 0 if k < 4 else 1
        return self.gates[kind] * dot(self.irrep[self.layer, kind], self.component(k))


def tall(row):
    return jnp.broadcast_to(row, (TALL, LANES)).astype(bf16)


def staged(stages, total):
    for time in range(total + len(stages) - 1):
        for late in reversed(range(len(stages))):
            if 0 <= time - late < total:
                stages[late](time - late)


def kernel(slabs, parts, block, *refs):
    halo_ref, inner_edges_ref, outer_edges_ref = refs[4:7]
    radial_out_ref, state_ref = refs[12], refs[17]
    _, paths, part, breadth = radial_out_ref.shape
    atoms = state_ref.shape[2]
    total = inner_edges_ref.shape[1] + outer_edges_ref.shape[1]
    rows = 9 * part
    *refs, sems = refs
    held = refs[-ARRAYS:]
    loads = [
        pltpu.make_async_copy(source, target, sems.at[i])
        for i, (source, target) in enumerate(zip(refs[3 : 3 + ARRAYS], held, strict=True))
    ]
    pl.run_scoped(
        functools.partial(program, slabs, parts, block, loads, *refs[:3], *held, *refs[3 + ARRAYS : -ARRAYS]),
        pltpu.VMEM((rows, block), bf16),
        pltpu.VMEM((rows, block), bf16),
        pltpu.VMEM((paths * part, total), bf16),
        pltpu.VMEM((2, breadth, block), bf16),
        pltpu.VMEM((2, 3 * part, block), bf16),
        pltpu.VMEM((2, part, block), bf16),
        pltpu.VMEM((rows, atoms), bf16),
        pltpu.VMEM((rows, 2 * halo_ref.shape[1]), bf16),
        pltpu.VMEM((2, part, atoms), bf16),
        pltpu.VMEM((3 * part, breadth), bf16),
        pltpu.VMEM((atoms, LANES), bf16),
    )


def program(
    slabs,
    parts,
    block,
    loads,
    live_ref,
    count_ref,
    energy_ref,
    species_ref,
    halo_ref,
    inner_edges_ref,
    outer_edges_ref,
    inner_vec_ref,
    outer_vec_ref,
    embed_ref,
    radial_in_ref,
    radial_mid_ref,
    radial_out_ref,
    mix_ref,
    scalar_ref,
    irrep_ref,
    readout_ref,
    state_out_ref,
    atom_ref,
    mean_ref,
    state_ref,
    state_sem,
    acc_ref,
    other_ref,
    basis_ref,
    geo_ref,
    dense_ref,
    flat_ref,
    agg_ref,
    all_ref,
    send_ref,
    land_ref,
    kind_send_ref,
    kind_land_ref,
    energies_ref,
    kind_send,
    kind_recv,
    agg_send,
    agg_recv,
    halo_send,
    halo_recv,
    energy_send,
    energy_recv,
    mess_ref,
    source_ref,
    weight_ref,
    hidden_ref,
    lead_ref,
    origin_ref,
    table_ref,
    halo_table_ref,
    first_table_ref,
    paths_ref,
    number_ref,
):
    part = mix_ref.shape[2]
    chans, atoms = state_ref.shape[1:]
    inner_total = inner_edges_ref.shape[1]
    held = halo_ref.shape[1]
    orders = radial_in_ref.shape[1]
    sub = min(SUB, block)
    for load in loads:
        load.start()
    for load in loads[:2]:
        load.wait()
    greet(others("chan", parts) + others("slab", slabs))

    values = jnp.broadcast_to(species_ref[...].astype(f32), (16, atoms)).astype(bf16)
    for side in range(2):
        kind_send_ref[side] = dot(values, onehot_rows(halo_ref[side : side + 1], atoms))[0:8]
    kind_copies = send_halo(kind_send_ref, kind_land_ref, kind_send, kind_recv, slabs)

    number_ref[...] = number_rows(atoms)
    acc_ref[...] = jnp.zeros_like(acc_ref)
    other_ref[...] = jnp.zeros_like(other_ref)
    lists = (
        (inner_edges_ref, inner_vec_ref, 0, live_ref[0, 0]),
        (outer_edges_ref, outer_vec_ref, inner_total, live_ref[0, 1]),
    )

    def geometry(which):
        _, vec_ref, base, _ = lists[which]
        chunk = 8 * LANES
        many = math.gcd(4, vec_ref.shape[1] // chunk)

        def body(step, carry):
            for part in range(many):
                piece(step * many + part, dense_ref.at[part], flat_ref.at[part])
            return carry

        def piece(step, dense_ref, flat_ref):
            offset = pl.multiple_of(step * chunk, chunk)
            for j in range(8):
                cols = pl.ds(pl.multiple_of(offset + j * LANES, LANES), LANES)
                for axis in range(3):
                    dense_ref[axis * 8 + j : axis * 8 + j + 1] = vec_ref[axis : axis + 1, cols]
            squared, inverse, x, y, z = unit([dense_ref[8 * axis : 8 * axis + 8] for axis in range(3)])
            rows = bessel_rows(squared, inverse, orders) + [x, y, z] + harmonics(x, y, z)
            for k, row in enumerate(rows):
                flat_ref[8 * k : 8 * k + 8] = row
            for j in range(8):
                cols = pl.ds(pl.multiple_of(base + offset + j * LANES, LANES), LANES)
                basis_ref[:, cols] = flat_ref[pl.ds(j, orders, stride=8)].astype(bf16)
                geo_ref[:, cols] = flat_ref[pl.ds(8 * orders + j, 8, stride=8)]

        lax.fori_loop(0, vec_ref.shape[1] // (many * chunk), body, 0)

    def hidden(layer, entry, place):
        hidden_ref[0] = silu(dot(entry, basis_ref[:, place])).astype(bf16)
        hidden_ref[1] = silu(dot(radial_mid_ref[layer], hidden_ref[0])).astype(bf16)

    subs = block // sub

    def scatter(which, step, j, into):
        edges_ref, _, _, live = lists[which]
        offset = step * block + j * sub
        lanes = lax.broadcasted_iota(jnp.int32, (1, sub), 1) + offset
        target = jnp.where(lanes < live, edges_ref[1:2, offset : offset + sub], -1)
        into[...] += dot_nt(mess_ref[:, j * sub : (j + 1) * sub], onehot_tiles(target, number_ref))

    def gather(which, step, j, features):
        offset = step * block + j * sub
        edges_ref = lists[which][0]
        return dot(features, onehot_tiles(edges_ref[0:1, offset : offset + sub], number_ref)).astype(bf16)

    def blocks(which):
        return [(which, step) for step in range(lists[which][0].shape[1] // block)]

    def first(now, then):
        halves = (range(subs // 2), range(subs // 2, subs))
        if then is not None:
            which, step = then
            slot = (lists[which][2] // block + step) % 2
            base = lists[which][2] + step * block
            hidden_ref[0] = silu(dot(entry, basis_ref[:, base : base + block])).astype(bf16)
        for half in range(2):
            if now is not None:
                for j in halves[half]:
                    combine_first(*now, j)
                    scatter(*now, j, (acc_ref, other_ref)[j % 2])
            if then is not None and half == 0:
                hidden_ref[1] = silu(dot(radial_mid_ref[0], hidden_ref[0])).astype(bf16)
        if then is not None:
            for j in range(subs):
                origin_ref[slot, :, j * sub : (j + 1) * sub] = gather(which, step, j, first_table_ref[which])
            lead_ref[slot] = dot(paths_ref[...], hidden_ref[1]).astype(bf16)

    def combine_first(which, step, j):
        start = lists[which][2] + step * block + j * sub
        slot = (lists[which][2] // block + step) % 2
        geo = geo_ref[:, start : start + sub]
        for lane in range(0, sub, LANES):
            cols = slice(j * sub + lane, j * sub + lane + LANES)
            around = [tall(geo[k : k + 1, lane : lane + LANES]) for k in range(8)]
            for low in range(0, part, TALL):
                held = origin_ref[slot, low : low + TALL, cols]

                def lead(k):
                    return lead_ref[slot, k * part + low : k * part + low + TALL, cols] * held

                def put(k, value):
                    mess_ref[k * part + low : k * part + low + TALL, cols] = value

                put(0, lead(0))
                for k, (low_k, high_k) in enumerate(GROUPS[1:]):
                    value = lead(1 + k)
                    for i in range(low_k, high_k):
                        put(i, value * around[i - 1])

    def second(which):
        features_ref = (table_ref, halo_table_ref)[which]

        def fetch(i):
            step, j = divmod(i, subs)
            source_ref[:, j * sub : (j + 1) * sub] = gather(which, step, j, features_ref[...])

        def settle(i):
            step, j = divmod(i, subs)
            scatter(which, step, j, acc_ref)

        def combine(i):
            step, j = divmod(i, subs)
            start = lists[which][2] + step * block + j * sub
            geo = geo_ref[:, start : start + sub]
            for lane in range(0, sub, LANES):
                cols = slice(j * sub + lane, j * sub + lane + LANES)
                x, y, z, *q = [tall(geo[k : k + 1, lane : lane + LANES]) for k in range(8)]
                weighed = slice(start + lane, start + lane + LANES)
                for low in range(0, part, TALL):

                    def at(k):
                        return source_ref[k * part + low : k * part + low + TALL, cols]

                    def path(k):
                        return weight_ref[k * part + low : k * part + low + TALL, weighed]

                    def put(k, value):
                        mess_ref[k * part + low : k * part + low + TALL, cols] = value

                    s = at(0)
                    v = [at(k) for k in (1, 2, 3)]
                    t = [at(k) for k in (4, 5, 6, 7, 8)]
                    a, b, c = v[0] * x, v[1] * y, v[2] * z
                    flat = a + b
                    along = flat + c
                    pairs = [
                        (v[1] * z, v[2] * y),
                        (v[2] * x, v[0] * z),
                        (v[0] * y, v[1] * x),
                    ]
                    third = root_third * t[2]
                    grad = [
                        y * t[0] + z * t[3] + x * (t[4] - third),
                        x * t[0] + z * t[1] - y * (t[4] + third),
                        y * t[1] + x * t[3] + z * (third + third),
                    ]
                    tq = x * grad[0] + y * grad[1] + z * grad[2]
                    put(0, path(0) * s + path(1) * tq + path(2) * along)
                    ws = path(3) * s
                    w4, w5, w6 = path(4), path(5), path(6)
                    for k, side in enumerate((x, y, z)):
                        one, two = pairs[k]
                        put(1 + k, ws * side + w4 * v[k] + w5 * (one - two) + w6 * grad[k])
                    ws = path(7) * s
                    w8, w9 = path(8), path(9)
                    sums = [one + two for one, two in pairs]
                    sym = [sums[2], sums[0], (2.0 * root_third) * c - root_third * flat, sums[1], a - b]
                    for k in range(5):
                        put(4 + k, ws * q[k] + w8 * t[k] + w9 * sym[k])

        staged([fetch, combine, settle], len(blocks(which)) * subs)

    for load in loads[4:6]:
        load.wait()
    geometry(0)
    geometry(1)
    for i, load in enumerate(loads):
        if i not in (0, 1, 4, 5):
            load.wait()
    start = initial(embed_ref, species_ref[...])
    first_table_ref[0] = dot(mix_ref[0, 0], start.astype(bf16)).astype(bf16)
    for k, path in enumerate((0, 3, 7)):
        paths_ref[k * part : (k + 1) * part] = radial_out_ref[0, path]
    entry = turned(radial_in_ref[0])
    entry_next = turned(radial_in_ref[1])
    mixers = [turned(scalar_ref[layer]) for layer in range(2)]
    order = blocks(0) + blocks(1)
    met = len(blocks(0)) - 1
    first(None, order[0])
    for i, (now, then) in enumerate(zip(order, order[1:] + [None])):
        if i == met:
            for copy in kind_copies:
                copy.wait()
            kinds = jnp.concatenate([kind_land_ref[0, 0:1], kind_land_ref[1, 0:1]], axis=1).astype(jnp.int32)
            first_table_ref[1] = dot(mix_ref[0, 0], initial(embed_ref, kinds).astype(bf16)).astype(bf16)
        first(now, then)
    agg_ref[0] = ((acc_ref[...] + other_ref[...]) * neighbour_norm).astype(bf16)
    copies, component = exchange(agg_ref.at[0], all_ref.at[0], agg_send.at[0], agg_recv.at[0], parts)
    acc_ref[...] = jnp.zeros_like(acc_ref)
    paths = radial_out_ref.shape[1]

    def prepare(step, carry):
        whole = pl.ds(pl.multiple_of(step * block, block), block)
        hidden(1, entry_next, whole)
        for path in range(paths):
            weighed = dot(radial_out_ref[1, path], hidden_ref[1])
            if path in (1, 6, 9):
                weighed = weighed * half_root
            weight_ref[path * part : (path + 1) * part, whole] = weighed.astype(bf16)
        return carry

    lax.fori_loop(0, basis_ref.shape[1] // block, prepare, 0)
    for copy in copies:
        copy.wait_recv()
    picks = jnp.concatenate([onehot_rows(halo_ref[side : side + 1], atoms) for side in range(2)], axis=1)
    outs = Updates(settled(all_ref.at[0]), mixers[0], irrep_ref, 0)
    for k in range(9):
        out = outs[k]
        if k == 0:
            out += start
        state_ref[k] = out
        which = 0 if k == 0 else (1 if k < 4 else 2)
        table_ref[k * part : (k + 1) * part] = dot(mix_ref[1, which], out.astype(bf16)).astype(bf16)
    picked = dot(table_ref[...], picks).astype(bf16)
    for side in range(2):
        send_ref[side] = picked[:, side * held : (side + 1) * held]
    for copy in copies:
        copy.wait_send()
    halo_copies = send_halo(send_ref, land_ref, halo_send, halo_recv, slabs)

    second(0)
    for copy in halo_copies:
        copy.wait()
    for side in range(2):
        halo_table_ref[:, side * held : (side + 1) * held] = land_ref[side]
    second(1)
    agg_ref[1] = (acc_ref[...] * neighbour_norm).astype(bf16)
    copies, component = exchange(agg_ref.at[1], all_ref.at[1], agg_send.at[1], agg_recv.at[1], parts)
    lines = lax.broadcasted_iota(jnp.int32, (chans, chans), 0)
    across = lax.broadcasted_iota(jnp.int32, (chans, chans), 1)
    readout = jnp.sum(jnp.where(lines == across, readout_ref[...], 0.0), axis=1, keepdims=True)
    own = jnp.zeros((1, atoms), f32)
    for kind in range(energy_ref.shape[0]):
        own = jnp.where(species_ref[...] == kind, energy_ref[kind], own)
    lanes = lax.broadcasted_iota(jnp.int32, (1, atoms), 1)
    outs = Updates(component, mixers[1], irrep_ref, 1)
    out = state_ref[0] + outs[0]
    state_ref[0] = out
    total = jnp.sum(out * readout, axis=0, keepdims=True) + own
    total = jnp.where(lanes < count_ref[0, 0], total, 0.0)
    me = lax.axis_index("slab")
    energies_ref[me] = jnp.broadcast_to(jnp.sum(total, axis=1, keepdims=True), energies_ref.shape[1:])
    atom_ref[...] = total
    sums = [
        remote(energies_ref.at[me], energies_ref.at[me], energy_send.at[i], energy_recv.at[i], peer)
        for i, peer in enumerate(others("slab", slabs))
    ]
    for copy in sums:
        copy.start()
    writes = [pltpu.make_async_copy(state_ref.at[k], state_out_ref.at[k], state_sem.at[k]) for k in range(9)]
    for k in range(1, 9):
        state_ref[k] = state_ref[k] + outs[k]
        if k > 1:
            writes[k - 2].start()
    for copy in copies:
        copy.wait_send()
    for write in writes[7:]:
        write.start()
    for copy in sums:
        copy.wait()
    for write in writes:
        write.wait()
    mean_ref[...] = jnp.sum(energies_ref[...], axis=0)[0:1, 0:1] * (1.0 / (atoms * slabs))


def deliver(*refs):
    state_in, atom_in, mean_in, state_out, atom_out, mean_out, state, atom, mean, sems = refs
    pairs = [(state_in.at[k], state.at[k], state_out.at[k]) for k in range(state.shape[0])]
    pairs += [(atom_in, atom, atom_out), (mean_in, mean, mean_out)]
    loads = [pltpu.make_async_copy(a, b, sems.at[0, i]) for i, (a, b, _) in enumerate(pairs)]
    writes = [pltpu.make_async_copy(b, c, sems.at[1, i]) for i, (_, b, c) in enumerate(pairs)]
    for load in loads:
        load.start()
    for load, write in zip(loads, writes, strict=True):
        load.wait()
        write.start()
    for write in writes:
        write.wait()


vmem = pl.BlockSpec(memory_space=pltpu.VMEM)
anywhere = pl.BlockSpec(memory_space=pl.ANY)
smem = pl.BlockSpec(memory_space=pltpu.SMEM)


def local(
    species,
    atom_count,
    halo_index,
    edge_count,
    inner_edges,
    outer_edges,
    inner_vec,
    outer_vec,
    embed_table,
    radial_in,
    radial_mid,
    radial_out,
    mix_in,
    mix_scalar,
    mix_irrep,
    readout,
    species_energy,
):
    slabs = lax.axis_size("slab")
    parts = lax.axis_size("chan")
    atoms = species.shape[0]
    chans = embed_table.shape[0]
    part = mix_in.shape[2]
    basis = radial_in.shape[2]
    halo = halo_index[0]
    held = halo.shape[1]
    rows = 9 * part
    inner_total, outer_total = inner_edges.shape[1], outer_edges.shape[1]
    total = inner_total + outer_total
    shared = math.gcd(inner_total, outer_total)
    block = math.gcd(BLOCK, shared)
    dma = pltpu.SemaphoreType.DMA
    arrays = (
        species[None, :],
        halo,
        inner_edges,
        outer_edges,
        inner_vec,
        outer_vec,
        embed_table.T,
        jnp.swapaxes(radial_in, 1, 2),
        radial_mid,
        radial_out,
        mix_in,
        jnp.swapaxes(mix_scalar, 1, 2),
        mix_irrep,
        readout[None, :],
    )
    shapes = (
        jax.ShapeDtypeStruct((9, chans, atoms), f32),
        jax.ShapeDtypeStruct((1, atoms), f32),
        jax.ShapeDtypeStruct((1, 1), f32),
    )
    results = pl.pallas_call(
        functools.partial(kernel, slabs, parts, block),
        out_shape=shapes,
        in_specs=[smem] * 3 + [pl.BlockSpec(memory_space=pltpu.HBM)] * ARRAYS,
        out_specs=(anywhere, vmem, vmem),
        scratch_shapes=[
            pltpu.VMEM((9, chans, atoms), f32),
            dma((9,)),
            pltpu.VMEM((rows, atoms), f32),
            pltpu.VMEM((rows, atoms), f32),
            pltpu.VMEM((basis, total), bf16),
            pltpu.VMEM((8, total), f32),
            pltpu.VMEM((4, 24, LANES), f32),
            pltpu.VMEM((4, 8 * (basis + 8), LANES), f32),
            pltpu.VMEM((2, rows, atoms), bf16),
            pltpu.VMEM((2, parts, rows, atoms), bf16),
            pltpu.VMEM((2, rows, held), bf16),
            pltpu.VMEM((2, rows, held), bf16),
            pltpu.VMEM((2, 8, held), f32),
            pltpu.VMEM((2, 8, held), f32),
            pltpu.VMEM((slabs, 8, 128), f32),
            dma((2,)),
            dma((2,)),
            dma((2, parts - 1, 3)),
            dma((2, parts - 1, 3)),
            dma((2,)),
            dma((2,)),
            dma((slabs - 1,)),
            dma((slabs - 1,)),
            *[pltpu.VMEM(array.shape, array.dtype) for array in arrays],
            dma((ARRAYS,)),
        ],
        compiler_params=pltpu.CompilerParams(
            vmem_limit_bytes=60 * 1024 * 1024, collective_id=0, has_side_effects=True
        ),
        name="message_passing",
    )(
        edge_count,
        atom_count[None, :],
        species_energy,
        *arrays,
    )
    node_state, atom_energy, mean_energy = pl.pallas_call(
        deliver,
        out_shape=shapes,
        in_specs=[anywhere] * 3,
        out_specs=(anywhere,) * 3,
        scratch_shapes=[pltpu.VMEM(shape.shape, shape.dtype) for shape in shapes] + [dma((2, 11))],
        compiler_params=pltpu.CompilerParams(vmem_limit_bytes=60 * 1024 * 1024),
        name="deliver",
    )(*results)
    return (node_state, atom_energy[0], mean_energy[0, 0])


def solution(mesh):
    return jax.shard_map(
        local,
        mesh=mesh,
        in_specs=(
            P("slab"),
            P("slab"),
            P("slab", None, None),
            P("slab", None),
            P(None, "slab"),
            P(None, "slab"),
            P(None, "slab"),
            P(None, "slab"),
            P(),
            P(),
            P(),
            P(None, None, "chan", None),
            P(None, None, "chan", None),
            P(),
            P(),
            P(),
            P(),
        ),
        out_specs=(P(None, None, "slab"), P("slab"), P()),
        check_vma=False,
    )
```

```python
import functools
import math

import jax
import jax.numpy as jnp
from jax import lax
from jax.experimental import pallas as pl
from jax.experimental.pallas import tpu as pltpu
from jax.sharding import PartitionSpec as P

cutoff = 5.0
neighbour_norm = 1.0 / math.sqrt(48.0)
root_three = math.sqrt(3.0)
half_root = 0.5 * math.sqrt(3.0)
BLOCK, SUB = 4096, 512
root_third = 1.0 / math.sqrt(3.0)
TALL, LANES = 16, 128
ARRAYS = 14
GROUPS = ((0, 1), (1, 4), (4, 9))
f32 = jnp.float32
bf16 = jnp.bfloat16


def dot(a, b):
    return jnp.dot(a, b, preferred_element_type=f32)


def dot_nt(a, b):
    return lax.dot_general(a, b, (((1,), (1,)), ((), ())), preferred_element_type=f32)


def sigmoid(v):
    return 0.5 * jnp.tanh(0.5 * v) + 0.5


def silu(v):
    half = 0.5 * v
    return half * jnp.tanh(half) + half


def number_rows(rows):
    return lax.broadcasted_iota(jnp.int32, (rows, LANES), 0).astype(f32).astype(bf16)


def onehot_tiles(index, number_ref):
    rows = number_ref.shape[0]
    one, zero = jnp.ones((), bf16), jnp.zeros((), bf16)
    tiles = []
    for low in range(0, index.shape[1], LANES):
        part = index[:, low : low + LANES].astype(f32)
        part = jnp.broadcast_to(part, (rows, LANES)).astype(bf16)
        tiles.append(jnp.where(number_ref[...] == part, one, zero))
    return jnp.concatenate(tiles, axis=1)


def onehot_rows(index, rows):
    slots = lax.broadcasted_iota(jnp.int32, (rows, index.shape[1]), 0)
    return jnp.where(slots == index, 1.0, 0.0).astype(bf16)


def turned(matrix):
    return matrix.astype(f32).T.astype(bf16)


def initial(embed_ref, species_row):
    return dot(turned(embed_ref[...]), onehot_rows(species_row, embed_ref.shape[0]))


def unit(vec):
    x, y, z = vec
    squared = x * x + y * y + z * z
    inverse = lax.rsqrt(squared + 0.25)
    return squared, inverse, x * inverse, y * inverse, z * inverse


def bessel_rows(squared, inverse, orders):
    length = jnp.sqrt(squared)
    fraction = jnp.minimum(length * (1.0 / cutoff), 1.0)
    cube = fraction * fraction * fraction
    sixth = cube * cube
    envelope = 1.0 - sixth * (28.0 - fraction * (48.0 - 21.0 * fraction))
    half = length * (0.5 * math.pi / cutoff)
    h2 = half * half
    sine = 1.0
    cosine = 1.0
    for order in range(12, 0, -2):
        sine = 1.0 - sine * h2 * (1.0 / ((order + 1) * order))
        cosine = 1.0 - cosine * h2 * (1.0 / (order * (order - 1)))
    sine = sine * half
    twice_cos = 2.0 - 4.0 * sine * sine
    first = 2.0 * sine * cosine
    scale = math.sqrt(2.0 / cutoff) * inverse * envelope
    before, now = jnp.zeros_like(first), first * scale
    rows = []
    for _ in range(orders):
        rows.append(now)
        before, now = now, twice_cos * now - before
    return rows


def harmonics(x, y, z):
    return [
        root_three * x * y,
        root_three * y * z,
        0.5 * (2.0 * z * z - x * x - y * y),
        root_three * x * z,
        half_root * (x * x - y * y),
    ]


def radial(entry, mid, basis):
    hidden = silu(dot(entry, basis)).astype(bf16)
    return silu(dot(mid, hidden)).astype(bf16)


mesh_ids = pl.DeviceIdType.MESH


def greet(peers):
    barrier = pltpu.get_barrier_semaphore()
    for peer in peers:
        pl.semaphore_signal(barrier, inc=1, device_id=peer, device_id_type=mesh_ids)
    pl.semaphore_wait(barrier, len(peers))


def others(axis, total):
    me = lax.axis_index(axis)
    return [{axis: lax.rem(me + step, total)} for step in range(1, total)]


def beside(total):
    me = lax.axis_index("slab")
    return {"slab": lax.rem(me + total - 1, total)}, {"slab": lax.rem(me + 1, total)}


def remote(src, dst, send_sem, recv_sem, peer):
    return pltpu.make_async_remote_copy(
        src_ref=src,
        dst_ref=dst,
        send_sem=send_sem,
        recv_sem=recv_sem,
        device_id=peer,
        device_id_type=mesh_ids,
    )


def send_halo(send_ref, land_ref, send_sem, recv_sem, total):
    copies = [
        remote(send_ref.at[side], land_ref.at[1 - side], send_sem.at[side], recv_sem.at[side], peer)
        for side, peer in enumerate(beside(total))
    ]
    for copy in copies:
        copy.start()
    return copies


def exchange(agg_ref, all_ref, send_sem, recv_sem, total):
    part = agg_ref.shape[0] // 9
    me = lax.axis_index("chan")
    peers = others("chan", total)
    copies = []
    for k, (low, high) in enumerate(GROUPS):
        span = slice(low * part, high * part)
        for i, peer in enumerate(peers):
            copies.append(
                remote(agg_ref.at[span], all_ref.at[me, span], send_sem.at[i, k], recv_sem.at[i, k], peer)
            )
    for copy in copies:
        copy.start()
    all_ref[me] = agg_ref[...]

    def component(k):
        for group, (low, high) in enumerate(GROUPS):
            if k == low:
                for copy in copies[group * len(peers) : (group + 1) * len(peers)]:
                    copy.wait_recv()
        span = slice(k * part, (k + 1) * part)
        return jnp.concatenate([all_ref[i, span] for i in range(total)], axis=0)

    return copies, component


def settled(all_ref):
    part = all_ref.shape[1] // 9

    def component(k):
        span = slice(k * part, (k + 1) * part)
        return jnp.concatenate([all_ref[i, span] for i in range(all_ref.shape[0])], axis=0)

    return component


class Updates:
    def __init__(self, component, scalar, irrep_ref, layer):
        self.component, self.layer, self.irrep = component, layer, irrep_ref
        chans = irrep_ref.shape[2]
        y = dot(scalar, component(0))
        self.scalar = silu(y[:chans])
        self.gates = sigmoid(y[chans : 2 * chans]), sigmoid(y[2 * chans :])

    def __getitem__(self, k):
        if k == 0:
            return self.scalar
        kind = 0 if k < 4 else 1
        return self.gates[kind] * dot(self.irrep[self.layer, kind], self.component(k))


def tall(row):
    return jnp.broadcast_to(row, (TALL, LANES)).astype(bf16)


def staged(stages, total):
    for time in range(total + len(stages) - 1):
        for late in reversed(range(len(stages))):
            if 0 <= time - late < total:
                stages[late](time - late)


def kernel(slabs, parts, block, *refs):
    halo_ref, inner_edges_ref, outer_edges_ref = refs[4:7]
    radial_out_ref, state_ref = refs[12], refs[17]
    _, paths, part, breadth = radial_out_ref.shape
    atoms = state_ref.shape[2]
    total = inner_edges_ref.shape[1] + outer_edges_ref.shape[1]
    rows = 9 * part
    *refs, sems = refs
    held = refs[-ARRAYS:]
    loads = [
        pltpu.make_async_copy(source, target, sems.at[i])
        for i, (source, target) in enumerate(zip(refs[3 : 3 + ARRAYS], held, strict=True))
    ]
    pl.run_scoped(
        functools.partial(program, slabs, parts, block, loads, *refs[:3], *held, *refs[3 + ARRAYS : -ARRAYS]),
        pltpu.VMEM((rows, block), bf16),
        pltpu.VMEM((rows, block), bf16),
        pltpu.VMEM((paths * part, total), bf16),
        pltpu.VMEM((2, breadth, block), bf16),
        pltpu.VMEM((2, 3 * part, block), bf16),
        pltpu.VMEM((2, part, block), bf16),
        pltpu.VMEM((rows, atoms), bf16),
        pltpu.VMEM((rows, 2 * halo_ref.shape[1]), bf16),
        pltpu.VMEM((2, part, atoms), bf16),
        pltpu.VMEM((3 * part, breadth), bf16),
        pltpu.VMEM((atoms, LANES), bf16),
    )


def program(
    slabs,
    parts,
    block,
    loads,
    live_ref,
    count_ref,
    energy_ref,
    species_ref,
    halo_ref,
    inner_edges_ref,
    outer_edges_ref,
    inner_vec_ref,
    outer_vec_ref,
    embed_ref,
    radial_in_ref,
    radial_mid_ref,
    radial_out_ref,
    mix_ref,
    scalar_ref,
    irrep_ref,
    readout_ref,
    state_out_ref,
    atom_ref,
    mean_ref,
    state_ref,
    state_sem,
    acc_ref,
    other_ref,
    basis_ref,
    geo_ref,
    dense_ref,
    flat_ref,
    agg_ref,
    all_ref,
    send_ref,
    land_ref,
    kind_send_ref,
    kind_land_ref,
    energies_ref,
    kind_send,
    kind_recv,
    agg_send,
    agg_recv,
    halo_send,
    halo_recv,
    energy_send,
    energy_recv,
    mess_ref,
    source_ref,
    weight_ref,
    hidden_ref,
    lead_ref,
    origin_ref,
    table_ref,
    halo_table_ref,
    first_table_ref,
    paths_ref,
    number_ref,
):
    part = mix_ref.shape[2]
    chans, atoms = state_ref.shape[1:]
    inner_total = inner_edges_ref.shape[1]
    held = halo_ref.shape[1]
    orders = radial_in_ref.shape[1]
    sub = min(SUB, block)
    for load in loads:
        load.start()
    for load in loads[:2]:
        load.wait()
    greet(others("chan", parts) + others("slab", slabs))

    values = jnp.broadcast_to(species_ref[...].astype(f32), (16, atoms)).astype(bf16)
    for side in range(2):
        kind_send_ref[side] = dot(values, onehot_rows(halo_ref[side : side + 1], atoms))[0:8]
    kind_copies = send_halo(kind_send_ref, kind_land_ref, kind_send, kind_recv, slabs)

    number_ref[...] = number_rows(atoms)
    acc_ref[...] = jnp.zeros_like(acc_ref)
    other_ref[...] = jnp.zeros_like(other_ref)
    lists = (
        (inner_edges_ref, inner_vec_ref, 0, live_ref[0, 0]),
        (outer_edges_ref, outer_vec_ref, inner_total, live_ref[0, 1]),
    )

    def geometry(which, block_step):
        _, vec_ref, base, _ = lists[which]
        chunk = 8 * LANES
        many = block // chunk

        def piece(step, dense_ref, flat_ref):
            offset = step * chunk
            for j in range(8):
                cols = pl.ds(offset + j * LANES, LANES)
                for axis in range(3):
                    dense_ref[axis * 8 + j : axis * 8 + j + 1] = vec_ref[axis : axis + 1, cols]
            squared, inverse, x, y, z = unit([dense_ref[8 * axis : 8 * axis + 8] for axis in range(3)])
            rows = bessel_rows(squared, inverse, orders) + [x, y, z] + harmonics(x, y, z)
            for k, row in enumerate(rows):
                flat_ref[8 * k : 8 * k + 8] = row
            for j in range(8):
                cols = pl.ds(base + offset + j * LANES, LANES)
                basis_ref[:, cols] = flat_ref[pl.ds(j, orders, stride=8)].astype(bf16)
                geo_ref[:, cols] = flat_ref[pl.ds(8 * orders + j, 8, stride=8)]

        for part in range(many):
            piece(block_step * many + part, dense_ref.at[part], flat_ref.at[part])

    def hidden(layer, entry, place):
        hidden_ref[0] = silu(dot(entry, basis_ref[:, place])).astype(bf16)
        hidden_ref[1] = silu(dot(radial_mid_ref[layer], hidden_ref[0])).astype(bf16)

    subs = block // sub
    paths = radial_out_ref.shape[1]

    def scatter(which, step, j, into):
        edges_ref, _, _, live = lists[which]
        offset = step * block + j * sub
        lanes = lax.broadcasted_iota(jnp.int32, (1, sub), 1) + offset
        target = jnp.where(lanes < live, edges_ref[1:2, offset : offset + sub], -1)
        into[...] += dot_nt(mess_ref[:, j * sub : (j + 1) * sub], onehot_tiles(target, number_ref))

    def gather(which, step, j, features):
        offset = step * block + j * sub
        edges_ref = lists[which][0]
        return dot(features, onehot_tiles(edges_ref[0:1, offset : offset + sub], number_ref)).astype(bf16)

    def blocks(which):
        return [(which, step) for step in range(lists[which][0].shape[1] // block)]

    def weigh(path, place):
        weighed = dot(radial_out_ref[1, path], hidden_ref[1])
        if path in (1, 6, 9):
            weighed = weighed * half_root
        weight_ref[path * part : (path + 1) * part, place] = weighed.astype(bf16)

    def first(now, then, later):
        halves = (range(subs // 2), range(subs // 2, subs))
        if then is not None:
            which, step = then
            slot = (lists[which][2] // block + step) % 2
            base = lists[which][2] + step * block
            hidden_ref[0] = silu(dot(entry, basis_ref[:, base : base + block])).astype(bf16)
        else:
            hidden_ref[0] = silu(dot(entry_next, basis_ref[:, 0:block])).astype(bf16)
        if later is not None:
            geometry(*later)
        for half in range(2):
            for i, j in enumerate(halves[half]):
                if now is not None:
                    combine_first(*now, j)
                    scatter(*now, j, (acc_ref, other_ref)[j % 2])
                if then is None and half == 1:
                    for path in range(i, paths, len(halves[half])):
                        weigh(path, slice(0, block))
            if half == 0:
                hidden_ref[1] = silu(dot(radial_mid_ref[0 if then else 1], hidden_ref[0])).astype(bf16)
        if then is not None:
            for j in range(subs):
                origin_ref[slot, :, j * sub : (j + 1) * sub] = gather(which, step, j, first_table_ref[which])
            lead_ref[slot] = dot(paths_ref[...], hidden_ref[1]).astype(bf16)

    def combine_first(which, step, j):
        start = lists[which][2] + step * block + j * sub
        slot = (lists[which][2] // block + step) % 2
        geo = geo_ref[:, start : start + sub]
        for lane in range(0, sub, LANES):
            cols = slice(j * sub + lane, j * sub + lane + LANES)
            around = [tall(geo[k : k + 1, lane : lane + LANES]) for k in range(8)]
            for low in range(0, part, TALL):
                held = origin_ref[slot, low : low + TALL, cols]

                def lead(k):
                    return lead_ref[slot, k * part + low : k * part + low + TALL, cols] * held

                def put(k, value):
                    mess_ref[k * part + low : k * part + low + TALL, cols] = value

                put(0, lead(0))
                for k, (low_k, high_k) in enumerate(GROUPS[1:]):
                    value = lead(1 + k)
                    for i in range(low_k, high_k):
                        put(i, value * around[i - 1])

    def second(arrive):
        order = blocks(0) + blocks(1)

        def fetch(i):
            (which, step), j = order[i // subs], i % subs
            if i == len(blocks(0)) * subs:
                arrive()
            features_ref = (table_ref, halo_table_ref)[which]
            source_ref[:, j * sub : (j + 1) * sub] = gather(which, step, j, features_ref[...])

        def settle(i):
            (which, step), j = order[i // subs], i % subs
            scatter(which, step, j, acc_ref)

        def combine(i):
            (which, step), j = order[i // subs], i % subs
            start = lists[which][2] + step * block + j * sub
            geo = geo_ref[:, start : start + sub]
            for lane in range(0, sub, LANES):
                cols = slice(j * sub + lane, j * sub + lane + LANES)
                x, y, z, *q = [tall(geo[k : k + 1, lane : lane + LANES]) for k in range(8)]
                weighed = slice(start + lane, start + lane + LANES)
                for low in range(0, part, TALL):

                    def at(k):
                        return source_ref[k * part + low : k * part + low + TALL, cols]

                    def path(k):
                        return weight_ref[k * part + low : k * part + low + TALL, weighed]

                    def put(k, value):
                        mess_ref[k * part + low : k * part + low + TALL, cols] = value

                    s = at(0)
                    v = [at(k) for k in (1, 2, 3)]
                    t = [at(k) for k in (4, 5, 6, 7, 8)]
                    a, b, c = v[0] * x, v[1] * y, v[2] * z
                    flat = a + b
                    along = flat + c
                    pairs = [
                        (v[1] * z, v[2] * y),
                        (v[2] * x, v[0] * z),
                        (v[0] * y, v[1] * x),
                    ]
                    third = root_third * t[2]
                    grad = [
                        y * t[0] + z * t[3] + x * (t[4] - third),
                        x * t[0] + z * t[1] - y * (t[4] + third),
                        y * t[1] + x * t[3] + z * (third + third),
                    ]
                    tq = x * grad[0] + y * grad[1] + z * grad[2]
                    put(0, path(0) * s + path(1) * tq + path(2) * along)
                    ws = path(3) * s
                    w4, w5, w6 = path(4), path(5), path(6)
                    for k, side in enumerate((x, y, z)):
                        one, two = pairs[k]
                        put(1 + k, ws * side + w4 * v[k] + w5 * (one - two) + w6 * grad[k])
                    ws = path(7) * s
                    w8, w9 = path(8), path(9)
                    sums = [one + two for one, two in pairs]
                    sym = [sums[2], sums[0], (2.0 * root_third) * c - root_third * flat, sums[1], a - b]
                    for k in range(5):
                        put(4 + k, ws * q[k] + w8 * t[k] + w9 * sym[k])

        staged([fetch, combine, settle], len(order) * subs)

    for load in loads[4:6]:
        load.wait()
    geometry(*(blocks(0) + blocks(1))[0])
    for i, load in enumerate(loads):
        if i not in (0, 1, 4, 5):
            load.wait()
    start = initial(embed_ref, species_ref[...])
    first_table_ref[0] = dot(mix_ref[0, 0], start.astype(bf16)).astype(bf16)
    for k, path in enumerate((0, 3, 7)):
        paths_ref[k * part : (k + 1) * part] = radial_out_ref[0, path]
    entry = turned(radial_in_ref[0])
    entry_next = turned(radial_in_ref[1])
    mixers = [turned(scalar_ref[layer]) for layer in range(2)]
    order = blocks(0) + blocks(1)
    met = len(blocks(0)) - 1
    first(None, order[0], order[1])
    for i, (now, then) in enumerate(zip(order, order[1:] + [None])):
        if i == met:
            for copy in kind_copies:
                copy.wait()
            kinds = jnp.concatenate([kind_land_ref[0, 0:1], kind_land_ref[1, 0:1]], axis=1).astype(jnp.int32)
            first_table_ref[1] = dot(mix_ref[0, 0], initial(embed_ref, kinds).astype(bf16)).astype(bf16)
        first(now, then, order[i + 2] if i + 2 < len(order) else None)
    agg_ref[0] = ((acc_ref[...] + other_ref[...]) * neighbour_norm).astype(bf16)
    copies, component = exchange(agg_ref.at[0], all_ref.at[0], agg_send.at[0], agg_recv.at[0], parts)
    acc_ref[...] = jnp.zeros_like(acc_ref)

    def prepare(step, carry):
        whole = pl.ds(pl.multiple_of(step * block, block), block)
        hidden(1, entry_next, whole)
        for path in range(paths):
            weigh(path, whole)
        return carry

    lax.fori_loop(1, basis_ref.shape[1] // block, prepare, 0)
    for copy in copies:
        copy.wait_recv()
    picks = jnp.concatenate([onehot_rows(halo_ref[side : side + 1], atoms) for side in range(2)], axis=1)
    outs = Updates(settled(all_ref.at[0]), mixers[0], irrep_ref, 0)
    for k in range(9):
        out = outs[k]
        if k == 0:
            out += start
        state_ref[k] = out
        which = 0 if k == 0 else (1 if k < 4 else 2)
        table_ref[k * part : (k + 1) * part] = dot(mix_ref[1, which], out.astype(bf16)).astype(bf16)
    picked = dot(table_ref[...], picks).astype(bf16)
    for side in range(2):
        send_ref[side] = picked[:, side * held : (side + 1) * held]
    for copy in copies:
        copy.wait_send()
    halo_copies = send_halo(send_ref, land_ref, halo_send, halo_recv, slabs)

    def arrive():
        for copy in halo_copies:
            copy.wait()
        for side in range(2):
            halo_table_ref[:, side * held : (side + 1) * held] = land_ref[side]

    second(arrive)
    agg_ref[1] = (acc_ref[...] * neighbour_norm).astype(bf16)
    copies, component = exchange(agg_ref.at[1], all_ref.at[1], agg_send.at[1], agg_recv.at[1], parts)
    lines = lax.broadcasted_iota(jnp.int32, (chans, chans), 0)
    across = lax.broadcasted_iota(jnp.int32, (chans, chans), 1)
    readout = jnp.sum(jnp.where(lines == across, readout_ref[...], 0.0), axis=1, keepdims=True)
    own = jnp.zeros((1, atoms), f32)
    for kind in range(energy_ref.shape[0]):
        own = jnp.where(species_ref[...] == kind, energy_ref[kind], own)
    lanes = lax.broadcasted_iota(jnp.int32, (1, atoms), 1)
    outs = Updates(component, mixers[1], irrep_ref, 1)
    out = state_ref[0] + outs[0]
    state_ref[0] = out
    total = jnp.sum(out * readout, axis=0, keepdims=True) + own
    total = jnp.where(lanes < count_ref[0, 0], total, 0.0)
    me = lax.axis_index("slab")
    energies_ref[me] = jnp.broadcast_to(jnp.sum(total, axis=1, keepdims=True), energies_ref.shape[1:])
    atom_ref[...] = total
    sums = [
        remote(energies_ref.at[me], energies_ref.at[me], energy_send.at[i], energy_recv.at[i], peer)
        for i, peer in enumerate(others("slab", slabs))
    ]
    for copy in sums:
        copy.start()
    writes = [pltpu.make_async_copy(state_ref.at[k], state_out_ref.at[k], state_sem.at[k]) for k in range(9)]
    for k in range(1, 9):
        state_ref[k] = state_ref[k] + outs[k]
        if k > 1:
            writes[k - 2].start()
    for copy in copies:
        copy.wait_send()
    for write in writes[7:]:
        write.start()
    for copy in sums:
        copy.wait()
    for write in writes:
        write.wait()
    mean_ref[...] = jnp.sum(energies_ref[...], axis=0)[0:1, 0:1] * (1.0 / (atoms * slabs))


def deliver(*refs):
    state_in, atom_in, mean_in, state_out, atom_out, mean_out, state, atom, mean, sems = refs
    pairs = [(state_in.at[k], state.at[k], state_out.at[k]) for k in range(state.shape[0])]
    pairs += [(atom_in, atom, atom_out), (mean_in, mean, mean_out)]
    loads = [pltpu.make_async_copy(a, b, sems.at[0, i]) for i, (a, b, _) in enumerate(pairs)]
    writes = [pltpu.make_async_copy(b, c, sems.at[1, i]) for i, (_, b, c) in enumerate(pairs)]
    for load in loads:
        load.start()
    for load, write in zip(loads, writes, strict=True):
        load.wait()
        write.start()
    for write in writes:
        write.wait()


vmem = pl.BlockSpec(memory_space=pltpu.VMEM)
anywhere = pl.BlockSpec(memory_space=pl.ANY)
smem = pl.BlockSpec(memory_space=pltpu.SMEM)


def local(
    species,
    atom_count,
    halo_index,
    edge_count,
    inner_edges,
    outer_edges,
    inner_vec,
    outer_vec,
    embed_table,
    radial_in,
    radial_mid,
    radial_out,
    mix_in,
    mix_scalar,
    mix_irrep,
    readout,
    species_energy,
):
    slabs = lax.axis_size("slab")
    parts = lax.axis_size("chan")
    atoms = species.shape[0]
    chans = embed_table.shape[0]
    part = mix_in.shape[2]
    basis = radial_in.shape[2]
    halo = halo_index[0]
    held = halo.shape[1]
    rows = 9 * part
    inner_total, outer_total = inner_edges.shape[1], outer_edges.shape[1]
    total = inner_total + outer_total
    shared = math.gcd(inner_total, outer_total)
    block = math.gcd(BLOCK, shared)
    dma = pltpu.SemaphoreType.DMA
    arrays = (
        species[None, :],
        halo,
        inner_edges,
        outer_edges,
        inner_vec,
        outer_vec,
        embed_table.T,
        jnp.swapaxes(radial_in, 1, 2),
        radial_mid,
        radial_out,
        mix_in,
        jnp.swapaxes(mix_scalar, 1, 2),
        mix_irrep,
        readout[None, :],
    )
    shapes = (
        jax.ShapeDtypeStruct((9, chans, atoms), f32),
        jax.ShapeDtypeStruct((1, atoms), f32),
        jax.ShapeDtypeStruct((1, 1), f32),
    )
    results = pl.pallas_call(
        functools.partial(kernel, slabs, parts, block),
        out_shape=shapes,
        in_specs=[smem] * 3 + [pl.BlockSpec(memory_space=pltpu.HBM)] * ARRAYS,
        out_specs=(anywhere, vmem, vmem),
        scratch_shapes=[
            pltpu.VMEM((9, chans, atoms), f32),
            dma((9,)),
            pltpu.VMEM((rows, atoms), f32),
            pltpu.VMEM((rows, atoms), f32),
            pltpu.VMEM((basis, total), bf16),
            pltpu.VMEM((8, total), f32),
            pltpu.VMEM((block // (8 * LANES), 24, LANES), f32),
            pltpu.VMEM((block // (8 * LANES), 8 * (basis + 8), LANES), f32),
            pltpu.VMEM((2, rows, atoms), bf16),
            pltpu.VMEM((2, parts, rows, atoms), bf16),
            pltpu.VMEM((2, rows, held), bf16),
            pltpu.VMEM((2, rows, held), bf16),
            pltpu.VMEM((2, 8, held), f32),
            pltpu.VMEM((2, 8, held), f32),
            pltpu.VMEM((slabs, 8, 128), f32),
            dma((2,)),
            dma((2,)),
            dma((2, parts - 1, 3)),
            dma((2, parts - 1, 3)),
            dma((2,)),
            dma((2,)),
            dma((slabs - 1,)),
            dma((slabs - 1,)),
            *[pltpu.VMEM(array.shape, array.dtype) for array in arrays],
            dma((ARRAYS,)),
        ],
        compiler_params=pltpu.CompilerParams(
            vmem_limit_bytes=60 * 1024 * 1024, collective_id=0, has_side_effects=True
        ),
        name="message_passing",
    )(
        edge_count,
        atom_count[None, :],
        species_energy,
        *arrays,
    )
    node_state, atom_energy, mean_energy = pl.pallas_call(
        deliver,
        out_shape=shapes,
        in_specs=[anywhere] * 3,
        out_specs=(anywhere,) * 3,
        scratch_shapes=[pltpu.VMEM(shape.shape, shape.dtype) for shape in shapes] + [dma((2, 11))],
        compiler_params=pltpu.CompilerParams(vmem_limit_bytes=60 * 1024 * 1024),
        name="deliver",
    )(*results)
    return (node_state, atom_energy[0], mean_energy[0, 0])


def solution(mesh):
    return jax.shard_map(
        local,
        mesh=mesh,
        in_specs=(
            P("slab"),
            P("slab"),
            P("slab", None, None),
            P("slab", None),
            P(None, "slab"),
            P(None, "slab"),
            P(None, "slab"),
            P(None, "slab"),
            P(),
            P(),
            P(),
            P(None, None, "chan", None),
            P(None, None, "chan", None),
            P(),
            P(),
            P(),
            P(),
        ),
        out_specs=(P(None, None, "slab"), P("slab"), P()),
        check_vma=False,
    )
```
